32 devices in a mesh: dp: 2 (over x), sp: 4 (over z), tp: 4 (over y, core).
Axes of the slice: x: 2, y: 2, z: 4, core: 2. Of those that a mesh axis runs over, the one named last changes fastest.
Arguments:
- hidden: bfloat16 [256, 4096], P('dp'), parts along dimension 0
- new_pos: int32 [256], P('dp'), parts along dimension 0
- k_self: bfloat16 [256, 256, 8, 128], P('dp', 'sp', 'tp'), parts along dimension 0
- v_self: bfloat16 [256, 256, 8, 128], P('dp', 'sp', 'tp'), parts along dimension 0
- k_cross: bfloat16 [256, 128, 8, 128], P('dp', None, 'tp'), parts along dimension 0
- v_cross: bfloat16 [256, 128, 8, 128], P('dp', None, 'tp'), parts along dimension 0
- xvalid: int32 [256, 128], P('dp'), parts along dimension 0
- rowmask: int32 [256], P('dp'), parts along dimension 0
- self_attn_norm: bfloat16 [4096], replicated
- self_wq: bfloat16 [4096, 4096], P(None, 'tp')
- self_wk: bfloat16 [4096, 1024], P(None, 'tp')
- self_wv: bfloat16 [4096, 1024], P(None, 'tp')
- self_wo: bfloat16 [4096, 4096], P('tp')
- self_mlp_norm: bfloat16 [4096], replicated
- self_wgate: bfloat16 [4096, 12288], P(None, 'tp')
- self_wup: bfloat16 [4096, 12288], P(None, 'tp')
- self_wdown: bfloat16 [12288, 4096], P('tp')
- cross_attn_norm: bfloat16 [4096], replicated
- cross_wq: bfloat16 [4096, 4096], P(None, 'tp')
- cross_qnorm: bfloat16 [128], replicated
- cross_wo: bfloat16 [4096, 4096], P('tp')
- cross_gates: float32 [2], replicated
- cross_mlp_norm: bfloat16 [4096], replicated
- cross_wgate: bfloat16 [4096, 12288], P(None, 'tp')
- cross_wup: bfloat16 [4096, 12288], P(None, 'tp')
- cross_wdown: bfloat16 [12288, 4096], P('tp')
Outputs:
- output 1: bfloat16 [256, 4096], P('dp'), parts along dimension 0
- output 2: bfloat16 [256, 256, 8, 128], P('dp', 'sp', 'tp'), parts along dimension 0
- output 3: bfloat16 [256, 256, 8, 128], P('dp', 'sp', 'tp'), parts along dimension 0
There are 2 independent parts. The reference program is written for one: setup_inputs(seed, part) draws one part's arguments, and reference() takes and returns one part's arrays. A program takes and returns all parts, laid end to end along the dimension named above; an argument that names none is the same for every part.
All inputs are finite; a program needn't handle non-finite values.
Results may differ from the reference program's by a relative error of at most 0.0149378.
Values sent between devices are 32-bit elements.
A program may use at most 1 GiB of HBM per device.

```python
import math
import jax
import jax.numpy as jnp
from jax import lax

BATCH = 128
SEQ_LEN = 256
VIS_TOKENS = 128
HIDDEN = 4096
HEADS = 32
KV_HEADS = 8
HEAD_DIM = 128
MLP_DIM = 12288

GROUP_SIZE = HEADS // KV_HEADS
Q_WIDTH = HEADS * HEAD_DIM
KV_WIDTH = KV_HEADS * HEAD_DIM
NORM_EPS = 1e-5
ROPE_THETA = 500000.0
ROPE_FACTOR = 8.0
LOW_FREQ = 1.0
HIGH_FREQ = 4.0
ORIG_CTX = 8192.0
NEG_BIG = -1e30
KEY_SCALE = 1.6


def rope_freqs():
    inv_freq = 1.0 / (ROPE_THETA ** (jnp.arange(0, HEAD_DIM, 2).astype(jnp.float32) / HEAD_DIM))
    wavelen = 2.0 * math.pi / inv_freq
    smooth = (ORIG_CTX / wavelen - LOW_FREQ) / (HIGH_FREQ - LOW_FREQ)
    mid_freq = (1.0 - smooth) * inv_freq / ROPE_FACTOR + smooth * inv_freq
    scaled = jnp.where(wavelen > ORIG_CTX / LOW_FREQ, inv_freq / ROPE_FACTOR, mid_freq)
    return jnp.where(wavelen < ORIG_CTX / HIGH_FREQ, inv_freq, scaled)


def apply_rope(vectors, positions):
    half_dim = HEAD_DIM // 2
    angles = positions.astype(jnp.float32)[:, None] * rope_freqs()[None, :]
    cos_t = jnp.cos(angles)[:, None, :]
    sin_t = jnp.sin(angles)[:, None, :]
    first_half = vectors[..., :half_dim]
    second_half = vectors[..., half_dim:]
    return jnp.concatenate([first_half * cos_t - second_half * sin_t, second_half * cos_t + first_half * sin_t], axis=-1)


def rms_norm(values, gain_vec):
    vals32 = values.astype(jnp.float32)
    inv_rms = lax.rsqrt(jnp.mean(vals32 * vals32, axis=-1, keepdims=True) + NORM_EPS)
    return (vals32 * inv_rms * gain_vec.astype(jnp.float32)).astype(jnp.bfloat16)


def gated_mlp(normed, w_gate, w_up, w_down):
    gate_val = jnp.dot(normed, w_gate, preferred_element_type=jnp.float32).astype(jnp.bfloat16)
    up_val = jnp.dot(normed, w_up, preferred_element_type=jnp.float32).astype(jnp.bfloat16)
    hidden_act = (jax.nn.silu(gate_val.astype(jnp.float32)) * up_val.astype(jnp.float32)).astype(jnp.bfloat16)
    return jnp.dot(hidden_act, w_down, preferred_element_type=jnp.float32)


def attend_row(queries, key_rows, val_rows, valid_mask):
    scores = jnp.einsum('kgd,tkd->kgt', queries.astype(jnp.float32), key_rows.astype(jnp.float32)) * (HEAD_DIM ** -0.5)
    scores = jnp.where(valid_mask[None, None, :], scores, NEG_BIG)
    weights = jax.nn.softmax(scores, axis=-1)
    return jnp.einsum('kgt,tkd->kgd', weights, val_rows.astype(jnp.float32))


def attend_item(item):
    return attend_row(item[0], item[1], item[2], item[3])


def dense_weight(rand_key, rows, cols):
    return (jax.random.normal(rand_key, (rows, cols), jnp.float32) * (rows ** -0.5)).astype(jnp.bfloat16)


def norm_gain(rand_key, width, center):
    return (center + 0.35 * jax.random.normal(rand_key, (width,), jnp.float32)).astype(jnp.bfloat16)


def drifting_values(rand_key, length):
    noise_key, walk_key, dir_key = jax.random.split(rand_key, 3)
    noise_part = 0.6 * jax.random.normal(noise_key, (BATCH, length, KV_HEADS, HEAD_DIM), jnp.float32)
    walk_path = jnp.cumsum(jax.random.normal(walk_key, (BATCH, KV_HEADS, length), jnp.float32), axis=-1) * (length ** -0.5)
    direction = jax.random.normal(dir_key, (BATCH, KV_HEADS, HEAD_DIM), jnp.float32)
    return (noise_part + jnp.transpose(walk_path, (0, 2, 1))[:, :, :, None] * direction[:, None, :, :]).astype(jnp.bfloat16)


def setup_inputs(seed: int = 0, part: int = 0) -> dict:
    data_keys = jax.random.split(jax.random.fold_in(jax.random.key(seed), part), 12)
    weight_keys = jax.random.split(jax.random.key(seed + 1), 20)
    row_ids = jnp.arange(BATCH)
    new_pos = jax.random.randint(data_keys[0], (BATCH,), SEQ_LEN // 4, SEQ_LEN)
    new_pos = jnp.where(row_ids == 0, SEQ_LEN - 1, new_pos).astype(jnp.int32)
    rowmask = (jax.random.randint(data_keys[1], (BATCH,), 0, 4) > 0).astype(jnp.int32)
    rowmask = jnp.where(row_ids == 0, 1, jnp.where(row_ids == 1, 0, rowmask)).astype(jnp.int32)
    valid_len = jax.random.randint(data_keys[2], (BATCH,), VIS_TOKENS // 4, VIS_TOKENS + 1)
    valid_len = jnp.where(row_ids == 0, VIS_TOKENS, valid_len)
    xvalid = (jnp.arange(VIS_TOKENS)[None, :] < valid_len[:, None]).astype(jnp.int32)
    hidden = jax.random.normal(data_keys[3], (BATCH, HIDDEN), jnp.float32).astype(jnp.bfloat16)
    k_self = (KEY_SCALE * jax.random.normal(data_keys[4], (BATCH, SEQ_LEN, KV_HEADS, HEAD_DIM), jnp.float32)).astype(jnp.bfloat16)
    v_self = drifting_values(data_keys[5], SEQ_LEN)
    k_cross = (KEY_SCALE * jax.random.normal(data_keys[6], (BATCH, VIS_TOKENS, KV_HEADS, HEAD_DIM), jnp.float32)).astype(jnp.bfloat16)
    v_cross = drifting_values(data_keys[7], VIS_TOKENS)
    return dict(
        hidden=hidden,
        new_pos=new_pos,
        k_self=k_self,
        v_self=v_self,
        k_cross=k_cross,
        v_cross=v_cross,
        xvalid=xvalid,
        rowmask=rowmask,
        self_attn_norm=norm_gain(weight_keys[0], HIDDEN, 1.0),
        self_wq=dense_weight(weight_keys[1], HIDDEN, Q_WIDTH),
        self_wk=dense_weight(weight_keys[2], HIDDEN, KV_WIDTH),
        self_wv=dense_weight(weight_keys[3], HIDDEN, KV_WIDTH),
        self_wo=dense_weight(weight_keys[4], Q_WIDTH, HIDDEN),
        self_mlp_norm=norm_gain(weight_keys[5], HIDDEN, 1.0),
        self_wgate=dense_weight(weight_keys[6], HIDDEN, MLP_DIM),
        self_wup=dense_weight(weight_keys[7], HIDDEN, MLP_DIM),
        self_wdown=dense_weight(weight_keys[8], MLP_DIM, HIDDEN),
        cross_attn_norm=norm_gain(weight_keys[9], HIDDEN, 1.0),
        cross_wq=dense_weight(weight_keys[10], HIDDEN, Q_WIDTH),
        cross_qnorm=norm_gain(weight_keys[11], HEAD_DIM, 1.5),
        cross_wo=dense_weight(weight_keys[12], Q_WIDTH, HIDDEN),
        cross_gates=jax.random.uniform(weight_keys[13], (2,), jnp.float32, 0.5, 1.5),
        cross_mlp_norm=norm_gain(weight_keys[14], HIDDEN, 1.0),
        cross_wgate=dense_weight(weight_keys[15], HIDDEN, MLP_DIM),
        cross_wup=dense_weight(weight_keys[16], HIDDEN, MLP_DIM),
        cross_wdown=dense_weight(weight_keys[17], MLP_DIM, HIDDEN),
    )


def reference(hidden, new_pos, k_self, v_self, k_cross, v_cross, xvalid, rowmask,
              self_attn_norm, self_wq, self_wk, self_wv, self_wo, self_mlp_norm,
              self_wgate, self_wup, self_wdown, cross_attn_norm, cross_wq, cross_qnorm,
              cross_wo, cross_gates, cross_mlp_norm, cross_wgate, cross_wup, cross_wdown):
    normed = rms_norm(hidden, self_attn_norm)
    queries = jnp.dot(normed, self_wq, preferred_element_type=jnp.float32).astype(jnp.bfloat16)
    key_new = jnp.dot(normed, self_wk, preferred_element_type=jnp.float32).astype(jnp.bfloat16)
    val_new = jnp.dot(normed, self_wv, preferred_element_type=jnp.float32).astype(jnp.bfloat16)
    queries = apply_rope(queries.reshape(BATCH, HEADS, HEAD_DIM).astype(jnp.float32), new_pos).astype(jnp.bfloat16)
    key_new = apply_rope(key_new.reshape(BATCH, KV_HEADS, HEAD_DIM).astype(jnp.float32), new_pos).astype(jnp.bfloat16)
    val_new = val_new.reshape(BATCH, KV_HEADS, HEAD_DIM)
    slot_ids = jnp.arange(SEQ_LEN)
    hit_mask = (slot_ids[None, :] == new_pos[:, None])[:, :, None, None]
    k_new_cache = jnp.where(hit_mask, key_new[:, None], k_self)
    v_new_cache = jnp.where(hit_mask, val_new[:, None], v_self)
    seen_mask = slot_ids[None, :] <= new_pos[:, None]
    self_out = lax.map(attend_item, (queries.reshape(BATCH, KV_HEADS, GROUP_SIZE, HEAD_DIM), k_new_cache, v_new_cache, seen_mask))
    self_flat = self_out.astype(jnp.bfloat16).reshape(BATCH, Q_WIDTH)
    after_attn = (hidden.astype(jnp.float32) + jnp.dot(self_flat, self_wo, preferred_element_type=jnp.float32)).astype(jnp.bfloat16)
    mlp_out = gated_mlp(rms_norm(after_attn, self_mlp_norm), self_wgate, self_wup, self_wdown)
    after_mlp = (after_attn.astype(jnp.float32) + mlp_out).astype(jnp.bfloat16)
    normed = rms_norm(after_mlp, cross_attn_norm)
    cross_q = jnp.dot(normed, cross_wq, preferred_element_type=jnp.float32).astype(jnp.bfloat16)
    cross_q = rms_norm(cross_q.reshape(BATCH, HEADS, HEAD_DIM), cross_qnorm)
    cross_out = lax.map(attend_item, (cross_q.reshape(BATCH, KV_HEADS, GROUP_SIZE, HEAD_DIM), k_cross, v_cross, xvalid > 0))
    cross_flat = cross_out.astype(jnp.bfloat16).reshape(BATCH, Q_WIDTH)
    gate_vals = jnp.tanh(cross_gates.astype(jnp.float32))
    row_scale = rowmask.astype(jnp.float32)[:, None]
    cross_proj = jnp.dot(cross_flat, cross_wo, preferred_element_type=jnp.float32)
    after_cross = (after_mlp.astype(jnp.float32) + gate_vals[0] * row_scale * cross_proj).astype(jnp.bfloat16)
    xmlp_out = gated_mlp(rms_norm(after_cross, cross_mlp_norm), cross_wgate, cross_wup, cross_wdown)
    after_xmlp = (after_cross.astype(jnp.float32) + gate_vals[1] * row_scale * xmlp_out).astype(jnp.bfloat16)
    return (after_xmlp, k_new_cache, v_new_cache)
```

```python
import math
import jax
import jax.numpy as jnp
from jax import lax
from jax.experimental import pallas as pl
from jax.experimental.pallas import tpu as pltpu
from jax.sharding import PartitionSpec as P

NORM_EPS = 1e-5
ROPE_THETA = 500000.0
ROPE_FACTOR = 8.0
LOW_FREQ = 1.0
HIGH_FREQ = 4.0
ORIG_CTX = 8192.0
NEG_BIG = -1e30
F32 = jnp.float32
BF16 = jnp.bfloat16
I32 = jnp.int32
MESH = pl.DeviceIdType.MESH
ANY = pl.ANY
VMEM = pltpu.VMEM
SMEM = pltpu.SMEM
NS = 23
B = 128
R = 32
HR = 16
W = 4096
D = 128
HL = 8
QW = 1024
FF = 3072
SPAN = 64
NG = 4
HC = 512
QC = 256
SCALE = D ** -0.5
MAXV = 67043328
NT = (((1,), (1,)), ((), ()))
WIN = {'preferred_element_type': F32}
ORDER = (2, 1, 3, 0)


def iota(shape, axis):
    return lax.broadcasted_iota(I32, shape, axis)


def rotary_freqs(lane):
    inv = jnp.exp((lane % SPAN).astype(F32) * (-2.0 / D * math.log(ROPE_THETA)))
    wave = 2.0 * math.pi / inv
    smooth = (ORIG_CTX / wave - LOW_FREQ) / (HIGH_FREQ - LOW_FREQ)
    mid = (1.0 - smooth) * inv / ROPE_FACTOR + smooth * inv
    scaled = jnp.where(wave > ORIG_CTX / LOW_FREQ, inv / ROPE_FACTOR, mid)
    return jnp.where(wave < ORIG_CTX / HIGH_FREQ, inv, scaled)


def norm_rows(src, gain, dst, r0, rows):
    at = slice(r0, r0 + rows)
    total = jnp.zeros((rows, D), F32)
    for c in range(0, W, D):
        v = src[at, c:c + D].astype(F32)
        total = total + v * v
    inv = lax.rsqrt(jnp.sum(total, axis=-1, keepdims=True) / W + NORM_EPS)
    for c in range(0, W, D):
        g = gain[c // D:c // D + 1, :].astype(F32)
        dst[at, c:c + D] = (src[at, c:c + D].astype(F32) * inv * g).astype(BF16)


def big_dot(lhs, rhs_of, depth, step=1024):
    acc = None
    for k in range(0, depth, step):
        part = jnp.dot(lhs[:, k:k + step], rhs_of(k, step), **WIN)
        acc = part if acc is None else acc + part
    return acc


def self_kernel(pos_s, g1, pos_a, hid, wq, wk, wv, kc, vc, kout, vout, qout,
                hb, xb, wb, kb, vb, q3, kn, vn, cs, sn, pv, w_sem, c_sem, o_sem, p_sem):
    base = lax.axis_index('sp') * SPAN

    def wcopy(i):
        src = (wk, wv)[i] if i < 2 else wq.at[:, (i - 2) * QC:(i - 1) * QC]
        return pltpu.make_async_copy(src, wb.at[i], w_sem.at[i])

    def ccopy(j):
        r = pl.ds((j // 2) * R, R)
        src, dst = ((kc, kb), (vc, vb))[j % 2]
        return pltpu.make_async_copy(src.at[r], dst.at[r], c_sem.at[j])

    def ocopy(j):
        r = pl.ds((j // 2) * R, R)
        src, dst = ((kb, kout), (vb, vout))[j % 2]
        return pltpu.make_async_copy(src.at[r], dst.at[r], o_sem.at[j])

    pcopy = pltpu.make_async_copy(pos_a, pv, p_sem.at[0])
    hcopy = pltpu.make_async_copy(hid, hb, p_sem.at[1])
    qcopy = pltpu.make_async_copy(q3, qout, p_sem.at[2])
    pcopy.start()
    hcopy.start()
    for i in range(2):
        wcopy(i).start()
    for j in range(2 * NG):
        ccopy(j).start()
    for i in range(2, 6):
        wcopy(i).start()

    pcopy.wait()
    ri = iota((B, D), 0)
    ci = iota((B, D), 1)
    posf = jnp.broadcast_to(pv[...].astype(F32), (B, D))
    pos_col = jnp.sum(jnp.where(ri == ci, posf, 0.0), axis=1, keepdims=True)
    ang = pos_col * jnp.broadcast_to(rotary_freqs(iota((1, D), 1)), (B, D))
    cs[...] = jnp.cos(ang)
    sn[...] = jnp.sin(ang) * jnp.where(ci < SPAN, -1.0, 1.0)

    hcopy.wait()
    norm_rows(hb, g1, xb, 0, B)

    def project(i):
        wcopy(i).wait()
        y = big_dot(xb, lambda k, w: wb[i, k:k + w, :], W).astype(BF16).astype(F32)
        for h in range(2):
            t = y[:, h * D:(h + 1) * D]
            if i != 1:
                t = t * cs[...] + pltpu.roll(t, SPAN, 1) * sn[...]
            t = t.astype(BF16).astype(F32)
            if i > 1:
                q3[:, (i - 2) * 2 + h, :] = t
            else:
                (kn, vn)[i][h] = t

    project(0)
    project(1)
    row16 = iota((HR, D), 0)
    for j in range(NG):
        ccopy(2 * j).wait()
        ccopy(2 * j + 1).wait()

        def body(it, _):
            for u in range(HL):
                b = j * R + it * HL + u
                lp = pos_s[b] - base
                t0 = pl.multiple_of((jnp.clip(lp, 0, SPAN - 1) // HL) * HR, HR)
                hit = row16 + t0 - 2 * lp
                for buf, new in ((kb, kn), (vb, vn)):
                    old = buf[b, pl.ds(t0, HR), :].astype(F32)
                    upd = jnp.where(hit == 0, new[0, pl.ds(b, 1), :], jnp.where(hit == 1, new[1, pl.ds(b, 1), :], old))
                    buf[b, pl.ds(t0, HR), :] = upd.astype(BF16)
            return 0
        lax.fori_loop(0, R // HL, body, 0)
        ocopy(2 * j).start()
        ocopy(2 * j + 1).start()
    for i in range(2, 6):
        project(i)
    qcopy.start()
    for j in range(2 * NG):
        ocopy(j).wait()
    qcopy.wait()


def rest_kernel(pos_s, mask_s, gates, g2, g3, g4, qn, q_in, ks, vs, hid, xval, kc, vc,
                wo, wg1, wu1, wd1, wqc, woc, wg2, wu2, wd2, out,
                slots, qb, ob, orecv, hrow, h, x, act, o2, q3, kb, vb, xv, xl,
                p0, m0, s1, t1, rb1, rb2, rb3, rbq, fin,
                w_sem, m_sem, k_sem, sp_send, sp_recv, a_send, a_recv, y_send, y_recv,
                b_send, b_recv, z_send, z_recv, f_send, f_recv, e_send, e_recv):
    sp = lax.axis_index('sp')
    tp = lax.axis_index('tp')
    core = tp % 2
    ypos = tp // 2
    sib = {'tp': tp + 1 - 2 * core}
    ypeer = {'tp': (tp + 2) % 4}
    row0 = pl.multiple_of(sp * R, R)
    other = 1 - core

    def half_col(g, half):
        return pl.multiple_of(g * 1024 + half * HC, HC)

    def remote(src, dst, ssem, rsem, dev):
        return pltpu.make_async_remote_copy(src, dst, ssem, rsem, device_id=dev, device_id_type=MESH)

    def cols(ref, c):
        return ref.at[:, pl.ds(pl.multiple_of(c, QC), QC)]

    def start(src, dst, slot):
        pltpu.make_async_copy(src, dst, w_sem.at[slot]).start()

    def put_o(ref):
        def f(j, slot):
            for k in range(4):
                half = other if k < 2 else core
                start(cols(ref, half_col(j, half) + (k % 2) * QC), slots.at[slot, k * QW:(k + 1) * QW], slot)
        return f

    def put_gu(gate, up):
        def f(j, slot):
            for n, ref in enumerate((gate, up)):
                @pl.when(j % 2 == n)
                def _():
                    start(cols(ref, (j // 2) * QC), slots.at[slot], slot)
        return f

    def put_down(ref):
        def f(j, slot):
            k = j % 4
            half = jnp.where(k < 2, other, core)
            start(cols(ref, half_col(j // 4, half) + (k % 2) * QC), slots.at[slot, 0:FF], slot)
        return f

    def put_q(ref):
        def f(j, slot):
            start(cols(ref, j * QC), slots.at[slot], slot)
        return f

    segs = []
    pos = 0
    for count, f in ((4, put_o(wo)), (24, put_gu(wg1, wu1)), (16, put_down(wd1)), (4, put_q(wqc)),
                     (4, put_o(woc)), (24, put_gu(wg2, wu2)), (16, put_down(wd2))):
        segs.append((pos, pos + count, f))
        pos += count

    def issue(i, lo, hi):
        for a, b, f in segs:
            if a <= lo and b >= hi:
                f(i - a, lax.rem(i, NS))
            elif a < hi and b > lo:
                @pl.when((i >= a) & (i < b))
                def _():
                    f(i - a, lax.rem(i, NS))

    def wait_item(i, depth=W):
        slot = lax.rem(i, NS)
        pltpu.make_async_copy(cols(wqc, 0).at[0:depth], slots.at[slot, 0:depth], w_sem.at[slot]).wait()
        return slot

    def refill(i, lo, hi):
        issue(i + NS, lo + NS, hi + NS)

    def dest_of(n):
        return (sp + ORDER[n % NG]) % NG

    def kv_self(n):
        r = pl.ds(pl.multiple_of(dest_of(n) * R + (n // NG) * HR, HR), HR)
        return [pltpu.make_async_copy(src.at[r], dst.at[n % NG], k_sem.at[i, n % NG])
                for i, (src, dst) in enumerate(((ks, kb), (vs, vb)))]

    def kv_cross(n):
        r = pl.ds(pl.multiple_of(row0 + (n // 2) * HR, HR), HR)
        return [pltpu.make_async_copy(src.at[r, n % 2], dst.at[n], k_sem.at[i, n])
                for i, (src, dst) in enumerate(((kc, kb), (vc, vb)))]

    def go(cs):
        for c in cs:
            c.start()

    def fin_wait(cs):
        for c in cs:
            c.wait()

    qcopy = pltpu.make_async_copy(q_in, qb, m_sem.at[0])
    hcopy = pltpu.make_async_copy(hid.at[pl.ds(row0, R)], hrow, m_sem.at[1])
    xcopy = pltpu.make_async_copy(xval.at[pl.ds(row0, R)], xv, m_sem.at[2])
    go([qcopy])
    for n in range(NG):
        go(kv_self(n))
    go([hcopy, xcopy])

    def fill(i, _):
        issue(i, 0, NS)
        return 0
    lax.fori_loop(0, NS, fill, 0)

    barrier = pltpu.get_barrier_semaphore()
    for dev in [{'sp': (sp + d) % NG} for d in ORDER[:3]] + [sib, ypeer]:
        pl.semaphore_signal(barrier, inc=1, device_id=dev, device_id_type=MESH)
    pl.semaphore_wait(barrier, 5)

    lane = iota((HL, D), 1)
    par = (lane % 2) == (iota((HL, D), 0) // 4)

    def scores(q, k):
        return lax.dot_general(q.astype(BF16), k, NT, **WIN) * SCALE

    def sp_copy(n):
        d = ORDER[n % NG]
        half = n // NG
        return remote(ob.at[d, half], orecv.at[sp, half], sp_send.at[half, d], sp_recv.at[half, d],
                      {'sp': dest_of(n)})

    def attend_stage(n):
        half = n // NG
        d = ORDER[n % NG]
        fin_wait(kv_self(n))
        first = dest_of(n) * R + half * HR
        slot = n % NG

        def body(it, st):
            res = []
            for u in range(HL):
                v = it * HL + u
                lp = pos_s[first + v] - sp * SPAN
                s = scores(qb[first + v], kb[slot, v])
                ok = par & (lane <= 2 * lp + 1)
                s = jnp.where(ok, s, NEG_BIG)
                m = jnp.max(s, axis=-1, keepdims=True)
                p = jnp.where(ok, jnp.exp(s - m), 0.0)
                res.append((m, jnp.sum(p, axis=-1, keepdims=True), p))
            for u in range(HL):
                v = it * HL + u
                m, l, p = res[u]
                o = jnp.dot(p.astype(BF16), vb[slot, v], **WIN)
                if d:
                    ob[d, half, v] = o
                else:
                    orecv[sp, half, v] = o
                st = jnp.where(lane == v, m, jnp.where(lane == HR + v, l, st))
            return st
        st = lax.fori_loop(0, HR // HL, body, jnp.zeros((HL, D), F32))
        if d:
            ob[d, half, HR] = st
            sp_copy(n).start()
        else:
            orecv[sp, half, HR] = st

    def combine(half):
        for n in range(NG * half, NG * half + 3):
            sp_copy(n).wait_recv()
        st = [orecv[s, half, HR] for s in range(NG)]
        gm = jnp.maximum(jnp.maximum(st[0], st[1]), jnp.maximum(st[2], st[3]))
        fac = [jnp.exp(v - gm) for v in st]
        tot = jnp.zeros((HL, D), F32)
        for v, f in zip(st, fac):
            tot = tot + pltpu.roll(v, D - HR, 1) * f
        wts = [f / tot for f in fac]
        for r in range(HR):
            acc = jnp.zeros((HL, D), F32)
            for s in range(NG):
                acc = acc + orecv[s, half, r] * wts[s][:, r:r + 1]
            q3[half * HR + r] = acc
        flatten(half)

    def flatten(half):
        at = slice(half * HR, half * HR + HR)
        for hh in range(HL):
            o2[at, hh * D:(hh + 1) * D] = q3[at, hh, :].astype(BF16)

    def d2d(k, g, half):
        at = pl.ds(half * HR, HR)
        return remote(p0.at[g, at], rb1.at[k, g, at], a_send.at[k, g, half], a_recv.at[k, g, half], sib)

    def ycp(k, g, half):
        at = pl.ds(half * HR, HR)
        return remote(s1.at[g, at], rb2.at[k, g, at], y_send.at[k, g, half], y_recv.at[k, g, half], ypeer)

    def back(k, g, half):
        at = pl.ds(half * HR, HR)
        return remote(t1.at[g, at], rb3.at[k, g, at], b_send.at[k, g, half], b_recv.at[k, g, half], sib)

    def add_core(k, g, half):
        at = slice(half * HR, half * HR + HR)
        d2d(k, g, half).wait_recv()
        s1[g, at] = m0[g, at] + rb1[k, g, at]
        ycp(k, g, half).start()

    def add_chip(k, g, half):
        at = slice(half * HR, half * HR + HR)
        ycp(k, g, half).wait_recv()
        t1[g, at] = s1[g, at] + rb2[k, g, at]
        back(k, g, half).start()

    def settle(k, half, scale_col):
        at = slice(half * HR, half * HR + HR)

        def upd(src, c0):
            to = pl.ds(c0, HC)
            v = src if scale_col is None else scale_col[at] * src
            h[at, to] = (h[at, to] + v).astype(BF16).astype(F32)
        for g in range(NG):
            upd(t1[g, at], half_col(g, core))
        for g in range(NG):
            back(k, g, half).wait_recv()
            upd(rb3[k, g, at], half_col(g, other))

    def drain(k):
        for g in range(NG):
            for half in range(2):
                d2d(k, g, half).wait_send()
                ycp(k, g, half).wait_send()
                back(k, g, half).wait_send()

    def o_products(k, base, half, last):
        at = slice(half * HR, half * HR + HR)
        for g in range(NG):
            i = base + g
            slot = i % NS
            if half == 0:
                wait_item(i)
            r = [big_dot(o2.at[at], lambda k_, w: slots[slot, n * QW + k_:n * QW + k_ + w, :], QW) for n in range(4)]
            p0[g, at] = jnp.concatenate(r[:2], axis=1)
            d2d(k, g, half).start()
            m0[g, at] = jnp.concatenate(r[2:], axis=1)
            if last:
                refill(i, i, i + 1)

    def down_product(base):
        def f(g, part):
            i = base + 4 * g + 2 * part
            r = []
            for n in range(2):
                slot = wait_item(i + n, FF)
                r.append(big_dot(act, lambda k, w: slots[slot, pl.ds(k, w), :], FF))
            for n in range(2):
                refill(i + n, base, base + 16)
            return jnp.concatenate(r, axis=1)
        return f

    def reduce_down(k, base):
        product = down_product(base)

        def body(g, _):
            p0[g] = product(g, 0)
            for half in range(2):
                d2d(k, g, half).start()
            m0[g] = product(g, 1)
            for half in range(2):
                add_core(k, g, half)
            return 0
        lax.fori_loop(0, NG, body, 0)

    def gate_up(base, gain):
        for half in range(2):
            norm_rows(h, gain, x, half * HR, HR)

        def body(j, _):
            i = base + 2 * j
            r = []
            for n in range(2):
                slot = wait_item(i + n)
                r.append(big_dot(x, lambda k, w: slots[slot, pl.ds(k, w), :], W).astype(BF16).astype(F32))
            for n in range(2):
                refill(i + n, base, base + 24)
            gv, uv = r
            act[:, pl.ds(pl.multiple_of(j * QC, QC), QC)] = (gv * (1.0 / (1.0 + jnp.exp(-gv))) * uv).astype(BF16)
            return 0
        lax.fori_loop(0, 12, body, 0)

    rid = iota((R, D), 0)
    maskv = jnp.zeros((R, D), F32)
    for r in range(R):
        maskv = jnp.where(rid == r, mask_s[row0 + r].astype(F32), maskv)
    mask_col = maskv[:, 0:1]

    fin_wait([qcopy])
    for n in range(2 * NG):
        attend_stage(n)
        if n < NG:
            go(kv_self(n + NG))
        else:
            go(kv_cross(n - NG))
    fin_wait([hcopy])
    for c in range(0, W, HC):
        h[:, c:c + HC] = hrow[:, c:c + HC].astype(F32)

    def groups(f, k, half):
        for g in range(NG):
            f(k, g, half)

    base = segs[0][0]
    combine(0)
    o_products(0, base, 0, False)
    groups(add_core, 0, 0)
    combine(1)
    o_products(0, base, 1, True)
    groups(add_chip, 0, 0)
    groups(add_core, 0, 1)
    settle(0, 0, None)
    groups(add_chip, 0, 1)
    settle(0, 1, None)
    drain(0)
    gate_up(segs[1][0], g2)

    reduce_down(1, segs[2][0])
    for half in range(2):
        groups(add_chip, 1, half)
    for half in range(2):
        settle(1, half, None)
    drain(1)

    for half in range(2):
        norm_rows(h, g3, x, half * HR, HR)
    for j in range(NG):
        i = segs[3][0] + j
        slot = wait_item(i)
        y = big_dot(x, lambda k, w: slots[slot, pl.ds(k, w), :], W).astype(BF16).astype(F32)
        refill(i, i, i + 1)
        for hh in range(2):
            t = y[:, hh * D:(hh + 1) * D]
            inv = lax.rsqrt(jnp.mean(t * t, axis=-1, keepdims=True) + NORM_EPS)
            q3[:, 2 * j + hh, :] = (t * inv * qn[...].astype(F32)).astype(BF16).astype(F32)
    fin_wait([xcopy])
    xlen = jnp.sum(jnp.where(xv[...] > 0, 1.0, 0.0), axis=-1, keepdims=True)
    xl[...] = jnp.broadcast_to(2.0 * xlen, (R, D))
    lane2 = iota((HL, 2 * D), 1)
    par2 = (lane2 % 2) == (iota((HL, 2 * D), 0) // 4)
    lanef = lane2.astype(F32)

    for half in range(2):
        fin_wait(kv_cross(2 * half) + kv_cross(2 * half + 1))

        def xbody(it, _):
            res = []
            for u in range(HL):
                v = it * HL + u
                b = half * HR + v
                s = jnp.concatenate([scores(q3[b], kb[2 * half + t, v]) for t in range(2)], axis=1)
                ok = par2 & (lanef < xl[pl.ds(b, 1), :][:, 0:1])
                s = jnp.where(ok, s, NEG_BIG)
                m = jnp.max(s, axis=-1, keepdims=True)
                p = jnp.where(ok, jnp.exp(s - m), 0.0)
                res.append((p, jnp.sum(p, axis=-1, keepdims=True)))
            for u in range(HL):
                v = it * HL + u
                p, l = res[u]
                o = sum(jnp.dot(p[:, t * D:(t + 1) * D].astype(BF16), vb[2 * half + t, v], **WIN) for t in range(2))
                q3[half * HR + v] = o / l
            return 0
        lax.fori_loop(0, HR // HL, xbody, 0)
        flatten(half)

    ga = jnp.tanh(jnp.full((R, 1), gates[0], F32)) * mask_col
    gm2 = jnp.tanh(jnp.full((R, 1), gates[1], F32)) * mask_col
    base = segs[4][0]
    for half in range(2):
        o_products(2, base, half, half == 1)
        groups(add_core, 2, half)
    for half in range(2):
        groups(add_chip, 2, half)
    for half in range(2):
        settle(2, half, ga)
    drain(2)
    gate_up(segs[5][0], g4)

    product = down_product(segs[6][0])

    def quarter(y):
        return pl.ds(pl.multiple_of(y * QC, QC), QC)

    def last_d2d(g):
        return remote(p0.at[g], rb1.at[3, g], a_send.at[3, g, 0], a_recv.at[3, g, 0], sib)

    def qcp(g):
        return remote(s1.at[g, :, quarter(1 - ypos)], rbq.at[g], y_send.at[3, g, 0], y_recv.at[3, g, 0], ypeer)

    def zcp(g, d):
        piece = fin.at[g, core, ypos, sp]
        return remote(piece, piece, z_send.at[g, d], z_recv.at[g, d], {'sp': (sp + d) % NG})

    def fcp(g):
        piece = fin.at[g, core, ypos]
        return remote(piece, piece, f_send.at[g], f_recv.at[g], ypeer)

    def ecp(g):
        piece = fin.at[g, core]
        return remote(piece, piece, e_send.at[g], e_recv.at[g], sib)

    def stage_q(g):
        qcp(g).wait_recv()
        c0 = pl.multiple_of(half_col(g, core) + ypos * QC, QC)
        t = s1[g, :, quarter(ypos)] + rbq[g]
        fin[g, core, ypos, sp] = (h[:, pl.ds(c0, QC)] + gm2 * t).astype(BF16).astype(F32)
        for d in ORDER[:3]:
            zcp(g, d).start()

    def stage_f(g):
        for d in ORDER[:3]:
            zcp(g, d).wait_recv()
        fcp(g).start()

    def stage_e(g):
        fcp(g).wait_recv()
        ecp(g).start()

    def body(g, _):
        p0[g] = product(g, 0)
        last_d2d(g).start()
        mine = product(g, 1)
        last_d2d(g).wait_recv()
        s1[g] = mine + rb1[3, g]
        qcp(g).start()

        @pl.when(g > 0)
        def _():
            stage_q(g - 1)

        @pl.when(g > 1)
        def _():
            stage_f(g - 2)
        return 0
    lax.fori_loop(0, NG, body, 0)
    stage_q(3)
    stage_f(2)
    stage_e(0)
    stage_e(1)
    stage_f(3)
    stage_e(2)
    stage_e(3)

    def emit(g, half):
        for yy in range(2):
            c = pl.multiple_of(half_col(g, half) + yy * QC, QC)
            for zz in range(NG):
                out[zz * R:(zz + 1) * R, pl.ds(c, QC)] = fin[g, half, yy, zz].astype(BF16)
    for g in range(NG):
        emit(g, core)
    for g in range(NG):
        ecp(g).wait_recv()
        emit(g, other)
    for n in range(2 * NG):
        if n % NG < 3:
            sp_copy(n).wait_send()
    for g in range(NG):
        for c in [last_d2d(g), qcp(g), fcp(g), ecp(g)] + [zcp(g, d) for d in ORDER[:3]]:
            c.wait_send()


def solution(mesh):
    cache_spec = P('dp', 'sp', 'tp', None)
    cross_spec = P('dp', None, 'tp', None)
    row_spec = P('dp', None)
    vec_spec = P('dp')
    full_spec = P(None)
    col_spec = P(None, 'tp')
    split_rows = P('tp', None)
    in_specs = (row_spec, vec_spec, cache_spec, cache_spec, cross_spec, cross_spec, row_spec, vec_spec,
                full_spec, col_spec, col_spec, col_spec, split_rows, full_spec, col_spec, col_spec, split_rows,
                full_spec, col_spec, full_spec, split_rows, full_spec, full_spec, col_spec, col_spec, split_rows)
    out_specs = (row_spec, cache_spec, cache_spec)
    vm = pl.BlockSpec(memory_space=VMEM)
    sm = pl.BlockSpec(memory_space=SMEM)
    an = pl.BlockSpec(memory_space=ANY)
    dma = pltpu.SemaphoreType.DMA

    def local_step(hidden, new_pos, k_self, v_self, k_cross, v_cross, xvalid, rowmask,
                   self_attn_norm, self_wq, self_wk, self_wv, self_wo, self_mlp_norm,
                   self_wgate, self_wup, self_wdown, cross_attn_norm, cross_wq, cross_qnorm,
                   cross_wo, cross_gates, cross_mlp_norm, cross_wgate, cross_wup, cross_wdown):
        kc = k_self.reshape(B, D, D)
        vc = v_self.reshape(B, D, D)
        cache = jax.ShapeDtypeStruct((B, D, D), BF16)
        kout, vout, q = pl.pallas_call(
            self_kernel,
            name='self_part',
            out_shape=(cache, cache, jax.ShapeDtypeStruct((B, HL, D), F32)),
            in_specs=[sm, vm] + [an] * 7,
            out_specs=(an, an, an),
            scratch_shapes=[VMEM((B, W), BF16), VMEM((B, W), BF16), VMEM((6, W, QC), BF16),
                            VMEM((B, D, D), BF16), VMEM((B, D, D), BF16),
                            VMEM((B, HL, D), F32), VMEM((2, B, D), F32), VMEM((2, B, D), F32),
                            VMEM((B, D), F32), VMEM((B, D), F32), VMEM((1, D), I32),
                            dma((6,)), dma((8,)), dma((8,)), dma((3,))],
            compiler_params=pltpu.CompilerParams(vmem_limit_bytes=MAXV),
        )(new_pos, self_attn_norm.reshape(R, D), new_pos[None, :], hidden, self_wq, self_wk, self_wv, kc, vc)

        part = VMEM((NG, R, HC), F32)
        parts3 = VMEM((3, NG, R, HC), F32)
        h4 = pl.pallas_call(
            rest_kernel,
            name='rest_part',
            out_shape=jax.ShapeDtypeStruct((B, W), BF16),
            in_specs=[sm, sm, sm, vm, vm, vm, vm] + [an] * 16,
            out_specs=vm,
            scratch_shapes=[
                VMEM((NS, W, QC), BF16), VMEM((B, HL, D), F32), VMEM((NG, 2, HR + 1, HL, D), F32),
                VMEM((NG, 2, HR + 1, HL, D), F32), VMEM((R, W), BF16),
                VMEM((R, W), F32), VMEM((R, W), BF16), VMEM((R, FF), BF16), VMEM((R, QW), BF16),
                VMEM((R, HL, D), F32), VMEM((NG, HR, D, D), BF16), VMEM((NG, HR, D, D), BF16),
                VMEM((R, D), I32), VMEM((R, D), F32),
                part, part, part, part,
                VMEM((4, NG, R, HC), F32), parts3, parts3,
                VMEM((NG, R, QC), F32), VMEM((NG, 2, 2, NG, R, QC), F32),
                dma((NS,)), dma((3,)), dma((2, NG)), dma((2, NG)), dma((2, NG)),
                dma((4, NG, 2)), dma((4, NG, 2)), dma((4, NG, 2)), dma((4, NG, 2)),
                dma((3, NG, 2)), dma((3, NG, 2)), dma((NG, NG)), dma((NG, NG)),
                dma((NG,)), dma((NG,)), dma((NG,)), dma((NG,))],
            compiler_params=pltpu.CompilerParams(collective_id=0, has_side_effects=True,
                                                 vmem_limit_bytes=MAXV),
        )(new_pos, rowmask, cross_gates, self_mlp_norm.reshape(R, D), cross_attn_norm.reshape(R, D),
          cross_mlp_norm.reshape(R, D), cross_qnorm[None, :], q, kout, vout, hidden, xvalid,
          k_cross.reshape(B, 2, D, D), v_cross.reshape(B, 2, D, D),
          self_wo, self_wgate, self_wup, self_wdown, cross_wq, cross_wo, cross_wgate, cross_wup, cross_wdown)
        return h4, kout.reshape(k_self.shape), vout.reshape(v_self.shape)

    return jax.shard_map(local_step, mesh=mesh, in_specs=in_specs, out_specs=out_specs, check_vma=False)
```

```python
import math
import jax
import jax.numpy as jnp
from jax import lax
from jax.experimental import pallas as pl
from jax.experimental.pallas import tpu as pltpu
from jax.sharding import PartitionSpec as P

NORM_EPS = 1e-5
ROPE_THETA = 500000.0
ROPE_FACTOR = 8.0
LOW_FREQ = 1.0
HIGH_FREQ = 4.0
ORIG_CTX = 8192.0
NEG_BIG = -1e30
F32 = jnp.float32
BF16 = jnp.bfloat16
I32 = jnp.int32
MESH = pl.DeviceIdType.MESH
ANY = pl.ANY
VMEM = pltpu.VMEM
SMEM = pltpu.SMEM
NP = 12
B = 128
R = 32
HR = 16
W = 4096
D = 128
HL = 8
QW = 1024
FF = 3072
SPAN = 64
NG = 4
HC = 512
QC = 256
SCALE = D ** -0.5
MAXV = 67043328
NT = (((1,), (1,)), ((), ()))
WIN = {'preferred_element_type': F32}
ORDER = (2, 1, 3, 0)


def iota(shape, axis):
    return lax.broadcasted_iota(I32, shape, axis)


def rotary_freqs(lane):
    inv = jnp.exp((lane % SPAN).astype(F32) * (-2.0 / D * math.log(ROPE_THETA)))
    wave = 2.0 * math.pi / inv
    smooth = (ORIG_CTX / wave - LOW_FREQ) / (HIGH_FREQ - LOW_FREQ)
    mid = (1.0 - smooth) * inv / ROPE_FACTOR + smooth * inv
    scaled = jnp.where(wave > ORIG_CTX / LOW_FREQ, inv / ROPE_FACTOR, mid)
    return jnp.where(wave < ORIG_CTX / HIGH_FREQ, inv, scaled)


def norm_rows(src, gain, dst, r0, rows):
    at = slice(r0, r0 + rows)
    total = jnp.zeros((rows, D), F32)
    for c in range(0, W, D):
        v = src[at, c:c + D].astype(F32)
        total = total + v * v
    inv = lax.rsqrt(jnp.sum(total, axis=-1, keepdims=True) / W + NORM_EPS)
    for c in range(0, W, D):
        g = gain[c // D:c // D + 1, :].astype(F32)
        dst[at, c:c + D] = (src[at, c:c + D].astype(F32) * inv * g).astype(BF16)


def big_dot(lhs, rhs_of, depth, step=1024):
    acc = None
    for k in range(0, depth, step):
        part = jnp.dot(lhs[:, k:k + step], rhs_of(k, step), **WIN)
        acc = part if acc is None else acc + part
    return acc


def self_kernel(pos_s, g1, pos_a, hid, wq, wk, wv, kc, vc, kout, vout, qout,
                hb, xb, wb, kb, vb, q3, kn, vn, cs, sn, pv, w_sem, c_sem, o_sem, p_sem):
    base = lax.axis_index('sp') * SPAN

    def wcopy(i):
        src = (wk, wv)[i] if i < 2 else wq.at[:, (i - 2) * QC:(i - 1) * QC]
        return pltpu.make_async_copy(src, wb.at[i], w_sem.at[i])

    def ccopy(j):
        r = pl.ds((j // 2) * R, R)
        src, dst = ((kc, kb), (vc, vb))[j % 2]
        return pltpu.make_async_copy(src.at[r], dst.at[r], c_sem.at[j])

    def ocopy(j):
        r = pl.ds((j // 2) * R, R)
        src, dst = ((kb, kout), (vb, vout))[j % 2]
        return pltpu.make_async_copy(src.at[r], dst.at[r], o_sem.at[j])

    pcopy = pltpu.make_async_copy(pos_a, pv, p_sem.at[0])
    hcopy = pltpu.make_async_copy(hid, hb, p_sem.at[1])
    qcopy = pltpu.make_async_copy(q3, qout, p_sem.at[2])
    pcopy.start()
    hcopy.start()
    for i in range(2):
        wcopy(i).start()
    for j in range(2 * NG):
        ccopy(j).start()
    for i in range(2, 6):
        wcopy(i).start()

    pcopy.wait()
    ri = iota((B, D), 0)
    ci = iota((B, D), 1)
    posf = jnp.broadcast_to(pv[...].astype(F32), (B, D))
    pos_col = jnp.sum(jnp.where(ri == ci, posf, 0.0), axis=1, keepdims=True)
    ang = pos_col * jnp.broadcast_to(rotary_freqs(iota((1, D), 1)), (B, D))
    cs[...] = jnp.cos(ang)
    sn[...] = jnp.sin(ang) * jnp.where(ci < SPAN, -1.0, 1.0)

    hcopy.wait()
    norm_rows(hb, g1, xb, 0, B)

    def project(i):
        wcopy(i).wait()
        y = big_dot(xb, lambda k, w: wb[i, k:k + w, :], W).astype(BF16).astype(F32)
        for h in range(2):
            t = y[:, h * D:(h + 1) * D]
            if i != 1:
                t = t * cs[...] + pltpu.roll(t, SPAN, 1) * sn[...]
            t = t.astype(BF16).astype(F32)
            if i > 1:
                q3[:, (i - 2) * 2 + h, :] = t
            else:
                (kn, vn)[i][h] = t

    project(0)
    project(1)
    row16 = iota((HR, D), 0)
    for j in range(NG):
        ccopy(2 * j).wait()
        ccopy(2 * j + 1).wait()

        def body(it, _):
            for u in range(HL):
                b = j * R + it * HL + u
                lp = pos_s[b] - base
                t0 = pl.multiple_of((jnp.clip(lp, 0, SPAN - 1) // HL) * HR, HR)
                hit = row16 + t0 - 2 * lp
                for buf, new in ((kb, kn), (vb, vn)):
                    old = buf[b, pl.ds(t0, HR), :].astype(F32)
                    upd = jnp.where(hit == 0, new[0, pl.ds(b, 1), :], jnp.where(hit == 1, new[1, pl.ds(b, 1), :], old))
                    buf[b, pl.ds(t0, HR), :] = upd.astype(BF16)
            return 0
        lax.fori_loop(0, R // HL, body, 0)
        ocopy(2 * j).start()
        ocopy(2 * j + 1).start()
    for i in range(2, 6):
        project(i)
    qcopy.start()
    for j in range(2 * NG):
        ocopy(j).wait()
    qcopy.wait()


def rest_kernel(pos_s, mask_s, gates, g2, g3, g4, qn, q_in, ks, vs, hid, xval, kc, vc,
                wo, wg1, wu1, wd1, wqc, woc, wg2, wu2, wd2, out,
                slots, qb, ob, orecv, h, x, act, o2, q3, kb, vb, xv, xl,
                p0, m0, s1, t1, rb1, rb2, rb3, rbq, fin,
                w_sem, m_sem, k_sem, sp_send, sp_recv, a_send, a_recv, y_send, y_recv,
                b_send, b_recv, z_send, z_recv, f_send, f_recv, e_send, e_recv):
    sp = lax.axis_index('sp')
    tp = lax.axis_index('tp')
    core = tp % 2
    ypos = tp // 2
    sib = {'tp': tp + 1 - 2 * core}
    ypeer = {'tp': (tp + 2) % 4}
    row0 = pl.multiple_of(sp * R, R)
    other = 1 - core

    def half_col(g, half):
        return pl.multiple_of(g * 1024 + half * HC, HC)

    def remote(src, dst, ssem, rsem, dev):
        return pltpu.make_async_remote_copy(src, dst, ssem, rsem, device_id=dev, device_id_type=MESH)

    def cols(ref, c):
        return ref.at[:, pl.ds(pl.multiple_of(c, QC), QC)]

    def start(src, dst, slot):
        pltpu.make_async_copy(src, dst, w_sem.at[slot]).start(priority=1)

    def put_o(ref):
        def f(j, slot):
            for n in range(2):
                for k in range(4):
                    c = half_col(2 * j + n, other if k < 2 else core) + (k % 2) * QC
                    start(cols(ref, c), slots.at[slot, n, k * QW:(k + 1) * QW], slot)
        return f

    def put_gu(gate, up):
        def f(j, slot):
            start(cols(gate, j * QC), slots.at[slot, 0], slot)
            start(cols(up, j * QC), slots.at[slot, 1], slot)
        return f

    def put_down(ref):
        def f(j, slot):
            part = j % 2
            c = half_col(j // 2, other + part * (core - other))
            for n in range(2):
                start(cols(ref, c + n * QC), slots.at[slot, n, 0:FF], slot)
        return f

    def put_q(ref):
        def f(j, slot):
            for n in range(2):
                start(cols(ref, (2 * j + n) * QC), slots.at[slot, n], slot)
        return f

    puts = (put_o(wo), put_gu(wg1, wu1), put_down(wd1), put_q(wqc), put_o(woc), put_gu(wg2, wu2), put_down(wd2))
    starts = [0]
    for count in (2, 12, 8, 2, 2, 12, 8):
        starts.append(starts[-1] + count)
    last_pair = starts.pop()

    def slot_of(seg, j):
        p = starts[seg] % NP + j
        if isinstance(p, int):
            return p % NP
        return jnp.where(p >= NP, p - NP, p)

    def wait_pair(seg, j, depth=W):
        slot = slot_of(seg, j)
        dst = slots.at[slot] if depth == W else slots.at[slot, :, 0:depth]
        pltpu.make_async_copy(dst, dst, w_sem.at[slot]).wait()
        return slot

    def refill(seg, j, first):
        p = starts[seg] + first + NP
        if p < last_pair:
            to = max(n for n in range(len(starts)) if starts[n] <= p)
            puts[to](j + (starts[seg] + NP - starts[to]), slot_of(seg, j))

    def sub_loops(seg, body):
        count = {1: 12, 5: 12}[seg]
        edges = sorted({0, count} | {e - NP - starts[seg] for e in starts + [last_pair] if 0 < e - NP - starts[seg] < count})
        for a, b in zip(edges, edges[1:]):
            def run(j, c, a=a):
                body(j, a)
                return c
            lax.fori_loop(a, b, run, 0)

    def dest_of(n):
        return (sp + ORDER[n % NG]) % NG

    def kv_self(n):
        r = pl.ds(pl.multiple_of(dest_of(n) * R + (n // NG) * HR, HR), HR)
        return [pltpu.make_async_copy(src.at[r], dst.at[n % NG], k_sem.at[i, n % NG])
                for i, (src, dst) in enumerate(((ks, kb), (vs, vb)))]

    def kv_cross(n):
        r = pl.ds(pl.multiple_of(row0 + (n // 2) * HR, HR), HR)
        return [pltpu.make_async_copy(src.at[r, n % 2], dst.at[n], k_sem.at[i, n])
                for i, (src, dst) in enumerate(((kc, kb), (vc, vb)))]

    def go(cs):
        for c in cs:
            c.start()

    def fin_wait(cs):
        for c in cs:
            c.wait()

    qcopy = pltpu.make_async_copy(q_in, qb, m_sem.at[0])
    hcopy = pltpu.make_async_copy(hid.at[pl.ds(row0, R)], x, m_sem.at[1])
    xcopy = pltpu.make_async_copy(xval.at[pl.ds(row0, R)], xv, m_sem.at[2])
    go([qcopy])
    for n in range(NG):
        go(kv_self(n))
    go([hcopy, xcopy])

    for j in range(2):
        puts[0](j, slot_of(0, j))

    def fill(j, _):
        puts[1](j, slot_of(1, j))
        return 0
    lax.fori_loop(0, NP - 2, fill, 0)

    barrier = pltpu.get_barrier_semaphore()
    for dev in [{'sp': (sp + d) % NG} for d in ORDER[:3]] + [sib, ypeer]:
        pl.semaphore_signal(barrier, inc=1, device_id=dev, device_id_type=MESH)
    pl.semaphore_wait(barrier, 5)

    lane = iota((HL, D), 1)
    par = (lane % 2) == (iota((HL, D), 0) // 4)

    def scores(q, k):
        return lax.dot_general(q.astype(BF16), k, NT, **WIN) * SCALE

    def sp_copy(n):
        d = ORDER[n % NG]
        half = n // NG
        return remote(ob.at[d, half], orecv.at[sp, half], sp_send.at[half, d], sp_recv.at[half, d],
                      {'sp': dest_of(n)})

    def attend_stage(n):
        half = n // NG
        d = ORDER[n % NG]
        fin_wait(kv_self(n))
        first = dest_of(n) * R + half * HR
        slot = n % NG

        def body(it, st):
            res = []
            for u in range(HL):
                v = it * HL + u
                lp = pos_s[first + v] - sp * SPAN
                s = scores(qb[first + v], kb[slot, v])
                ok = par & (lane <= 2 * lp + 1)
                s = jnp.where(ok, s, NEG_BIG)
                m = jnp.max(s, axis=-1, keepdims=True)
                p = jnp.where(ok, jnp.exp(s - m), 0.0)
                res.append((m, jnp.sum(p, axis=-1, keepdims=True), p))
            for u in range(HL):
                v = it * HL + u
                m, l, p = res[u]
                o = jnp.dot(p.astype(BF16), vb[slot, v], **WIN)
                if d:
                    ob[d, half, v] = o
                else:
                    orecv[sp, half, v] = o
                st = jnp.where(lane == v, m, jnp.where(lane == HR + v, l, st))
            return st
        st = lax.fori_loop(0, HR // HL, body, jnp.zeros((HL, D), F32))
        if d:
            ob[d, half, HR] = st
            sp_copy(n).start()
        else:
            orecv[sp, half, HR] = st

    def combine(half):
        for n in range(NG * half, NG * half + 3):
            sp_copy(n).wait_recv()
        st = [orecv[s, half, HR] for s in range(NG)]
        gm = jnp.maximum(jnp.maximum(st[0], st[1]), jnp.maximum(st[2], st[3]))
        fac = [jnp.exp(v - gm) for v in st]
        tot = jnp.zeros((HL, D), F32)
        for v, f in zip(st, fac):
            tot = tot + pltpu.roll(v, D - HR, 1) * f
        wts = [f / tot for f in fac]
        for r in range(HR):
            acc = jnp.zeros((HL, D), F32)
            for s in range(NG):
                acc = acc + orecv[s, half, r] * wts[s][:, r:r + 1]
            q3[half * HR + r] = acc
        flatten(half)

    def flatten(half):
        at = slice(half * HR, half * HR + HR)
        for hh in range(HL):
            o2[at, hh * D:(hh + 1) * D] = q3[at, hh, :].astype(BF16)

    def d2d(k, g, half):
        at = pl.ds(half * HR, HR)
        return remote(p0.at[g, at], rb1.at[k, g, at], a_send.at[k, g, half], a_recv.at[k, g, half], sib)

    def ycp(k, g, half):
        at = pl.ds(half * HR, HR)
        return remote(s1.at[g, at], rb2.at[k, g, at], y_send.at[k, g, half], y_recv.at[k, g, half], ypeer)

    def back(k, g, half):
        at = pl.ds(half * HR, HR)
        return remote(t1.at[g, at], rb3.at[k, g, at], b_send.at[k, g, half], b_recv.at[k, g, half], sib)

    def add_core(k, g, half):
        at = slice(half * HR, half * HR + HR)
        d2d(k, g, half).wait_recv()
        s1[g, at] = m0[g, at] + rb1[k, g, at]
        ycp(k, g, half).start()

    def add_chip(k, g, half):
        at = slice(half * HR, half * HR + HR)
        ycp(k, g, half).wait_recv()
        t1[g, at] = s1[g, at] + rb2[k, g, at]
        back(k, g, half).start()

    def settle(k, half, scale_col):
        at = slice(half * HR, half * HR + HR)

        def upd(src, c0):
            to = pl.ds(c0, HC)
            v = src if scale_col is None else scale_col[at] * src
            h[at, to] = (h[at, to] + v).astype(BF16).astype(F32)
        for g in range(NG):
            upd(t1[g, at], half_col(g, core))
        for g in range(NG):
            back(k, g, half).wait_recv()
            upd(rb3[k, g, at], half_col(g, other))

    def drain(k):
        for g in range(NG):
            for half in range(2):
                d2d(k, g, half).wait_send()
                ycp(k, g, half).wait_send()
                back(k, g, half).wait_send()

    def o_products(k, seg, half, last):
        at = slice(half * HR, half * HR + HR)
        for g in range(NG):
            slot = slot_of(seg, g // 2)
            if half == 0 and g % 2 == 0:
                wait_pair(seg, g // 2)
            r = [jnp.dot(o2[at, :], slots[slot, g % 2, n * QW:(n + 1) * QW, :], **WIN) for n in range(4)]
            p0[g, at] = jnp.concatenate(r[:2], axis=1)
            d2d(k, g, half).start()
            m0[g, at] = jnp.concatenate(r[2:], axis=1)
            if last and g % 2:
                refill(seg, g // 2, g // 2)

    def down_product(seg):
        def f(g, part):
            j = 2 * g + part
            slot = wait_pair(seg, j, FF)
            r = [big_dot(act, lambda k, w: slots[slot, n, pl.ds(k, w), :], FF) for n in range(2)]
            refill(seg, j, 0)
            return jnp.concatenate(r, axis=1)
        return f

    def reduce_down(k, seg):
        product = down_product(seg)

        def both(g):
            for half in range(2):
                add_core(k, g, half)

        def body(g, _):
            p0[g] = product(g, 0)
            for half in range(2):
                d2d(k, g, half).start()

            @pl.when(g > 0)
            def _():
                both(g - 1)
            m0[g] = product(g, 1)
            return 0
        lax.fori_loop(0, NG, body, 0)
        both(3)

    def gate_up(seg, gain):
        for half in range(2):
            norm_rows(h, gain, x, half * HR, HR)

        def body(j, first):
            slot = wait_pair(seg, j)
            gv, uv = [big_dot(x, lambda k, w: slots[slot, n, pl.ds(k, w), :], W).astype(BF16).astype(F32) for n in range(2)]
            refill(seg, j, first)
            act[:, pl.ds(pl.multiple_of(j * QC, QC), QC)] = (gv * (1.0 / (1.0 + jnp.exp(-gv))) * uv).astype(BF16)
        sub_loops(seg, body)

    rid = iota((R, D), 0)
    maskv = jnp.zeros((R, D), F32)
    for r in range(R):
        maskv = jnp.where(rid == r, mask_s[row0 + r].astype(F32), maskv)
    mask_col = maskv[:, 0:1]

    fin_wait([qcopy])
    for n in range(2 * NG):
        attend_stage(n)
        if n < NG:
            go(kv_self(n + NG))
        else:
            go(kv_cross(n - NG))
    fin_wait([hcopy])
    for c in range(0, W, HC):
        h[:, c:c + HC] = x[:, c:c + HC].astype(F32)

    def groups(f, k, half):
        for g in range(NG):
            f(k, g, half)

    combine(0)
    o_products(0, 0, 0, False)
    groups(add_core, 0, 0)
    combine(1)
    o_products(0, 0, 1, True)
    groups(add_chip, 0, 0)
    groups(add_core, 0, 1)
    settle(0, 0, None)
    groups(add_chip, 0, 1)
    settle(0, 1, None)
    drain(0)
    gate_up(1, g2)

    reduce_down(1, 2)
    for half in range(2):
        groups(add_chip, 1, half)
    for half in range(2):
        settle(1, half, None)
    drain(1)

    for half in range(2):
        norm_rows(h, g3, x, half * HR, HR)
    for j in range(2):
        slot = wait_pair(3, j)
        ys = [big_dot(x, lambda k, w: slots[slot, n, pl.ds(k, w), :], W).astype(BF16).astype(F32) for n in range(2)]
        refill(3, j, j)
        for hh in range(4):
            t = ys[hh // 2][:, hh % 2 * D:(hh % 2 + 1) * D]
            inv = lax.rsqrt(jnp.mean(t * t, axis=-1, keepdims=True) + NORM_EPS)
            q3[:, NG * j + hh, :] = (t * inv * qn[...].astype(F32)).astype(BF16).astype(F32)
    fin_wait([xcopy])
    xlen = jnp.sum(jnp.where(xv[...] > 0, 1.0, 0.0), axis=-1, keepdims=True)
    xl[...] = jnp.broadcast_to(2.0 * xlen, (R, D))
    lane2 = iota((HL, 2 * D), 1)
    par2 = (lane2 % 2) == (iota((HL, 2 * D), 0) // 4)
    lanef = lane2.astype(F32)

    for half in range(2):
        fin_wait(kv_cross(2 * half) + kv_cross(2 * half + 1))

        def xbody(it, _):
            res = []
            for u in range(HL):
                v = it * HL + u
                b = half * HR + v
                s = jnp.concatenate([scores(q3[b], kb[2 * half + t, v]) for t in range(2)], axis=1)
                ok = par2 & (lanef < xl[pl.ds(b, 1), :][:, 0:1])
                s = jnp.where(ok, s, NEG_BIG)
                m = jnp.max(s, axis=-1, keepdims=True)
                p = jnp.where(ok, jnp.exp(s - m), 0.0)
                res.append((p, jnp.sum(p, axis=-1, keepdims=True)))
            for u in range(HL):
                v = it * HL + u
                p, l = res[u]
                o = sum(jnp.dot(p[:, t * D:(t + 1) * D].astype(BF16), vb[2 * half + t, v], **WIN) for t in range(2))
                q3[half * HR + v] = o / l
            return 0
        lax.fori_loop(0, HR // HL, xbody, 0)
        flatten(half)

    ga = jnp.tanh(jnp.full((R, 1), gates[0], F32)) * mask_col
    gm2 = jnp.tanh(jnp.full((R, 1), gates[1], F32)) * mask_col
    for half in range(2):
        o_products(2, 4, half, half == 1)
        groups(add_core, 2, half)
    for half in range(2):
        groups(add_chip, 2, half)
    for half in range(2):
        settle(2, half, ga)
    drain(2)
    gate_up(5, g4)

    product = down_product(6)

    def quarter(y):
        return pl.ds(pl.multiple_of(y * QC, QC), QC)

    def last_d2d(g):
        return remote(p0.at[g], rb1.at[3, g], a_send.at[3, g, 0], a_recv.at[3, g, 0], sib)

    def qcp(g):
        return remote(s1.at[g, :, quarter(1 - ypos)], rbq.at[g], y_send.at[3, g, 0], y_recv.at[3, g, 0], ypeer)

    def zcp(g, d):
        piece = fin.at[g, core, ypos, sp]
        return remote(piece, piece, z_send.at[g, d], z_recv.at[g, d], {'sp': (sp + d) % NG})

    def fcp(g):
        piece = fin.at[g, core, ypos]
        return remote(piece, piece, f_send.at[g], f_recv.at[g], ypeer)

    def ecp(g):
        piece = fin.at[g, core]
        return remote(piece, piece, e_send.at[g], e_recv.at[g], sib)

    def stage_q(g):
        qcp(g).wait_recv()
        c0 = pl.multiple_of(half_col(g, core) + ypos * QC, QC)
        t = s1[g, :, quarter(ypos)] + rbq[g]
        fin[g, core, ypos, sp] = (h[:, pl.ds(c0, QC)] + gm2 * t).astype(BF16).astype(F32)
        for d in ORDER[:3]:
            zcp(g, d).start()

    def stage_f(g):
        for d in ORDER[:3]:
            zcp(g, d).wait_recv()
        fcp(g).start()

    def stage_e(g):
        fcp(g).wait_recv()
        ecp(g).start()

    def stage_c(g):
        last_d2d(g).wait_recv()
        s1[g] = m0[g] + rb1[3, g]
        qcp(g).start()

    def body(g, _):
        p0[g] = product(g, 0)
        last_d2d(g).start()

        @pl.when(g > 0)
        def _():
            stage_c(g - 1)
        m0[g] = product(g, 1)

        @pl.when(g > 1)
        def _():
            stage_q(g - 2)
        return 0
    lax.fori_loop(0, NG, body, 0)
    stage_c(3)
    stage_q(2)
    stage_f(0)
    stage_q(3)
    stage_f(1)
    stage_e(0)
    stage_f(2)
    stage_e(1)
    stage_f(3)
    stage_e(2)
    stage_e(3)

    def emit(g, half):
        for yy in range(2):
            c = pl.multiple_of(half_col(g, half) + yy * QC, QC)
            for zz in range(NG):
                out[zz * R:(zz + 1) * R, pl.ds(c, QC)] = fin[g, half, yy, zz].astype(BF16)
    for g in range(NG):
        emit(g, core)
    for g in range(NG):
        ecp(g).wait_recv()
        emit(g, other)
    for n in range(2 * NG):
        if n % NG < 3:
            sp_copy(n).wait_send()
    for g in range(NG):
        for c in [last_d2d(g), qcp(g), fcp(g), ecp(g)] + [zcp(g, d) for d in ORDER[:3]]:
            c.wait_send()


def solution(mesh):
    cache_spec = P('dp', 'sp', 'tp', None)
    cross_spec = P('dp', None, 'tp', None)
    row_spec = P('dp', None)
    vec_spec = P('dp')
    full_spec = P(None)
    col_spec = P(None, 'tp')
    split_rows = P('tp', None)
    in_specs = (row_spec, vec_spec, cache_spec, cache_spec, cross_spec, cross_spec, row_spec, vec_spec,
                full_spec, col_spec, col_spec, col_spec, split_rows, full_spec, col_spec, col_spec, split_rows,
                full_spec, col_spec, full_spec, split_rows, full_spec, full_spec, col_spec, col_spec, split_rows)
    out_specs = (row_spec, cache_spec, cache_spec)
    vm = pl.BlockSpec(memory_space=VMEM)
    sm = pl.BlockSpec(memory_space=SMEM)
    an = pl.BlockSpec(memory_space=ANY)
    dma = pltpu.SemaphoreType.DMA

    def local_step(hidden, new_pos, k_self, v_self, k_cross, v_cross, xvalid, rowmask,
                   self_attn_norm, self_wq, self_wk, self_wv, self_wo, self_mlp_norm,
                   self_wgate, self_wup, self_wdown, cross_attn_norm, cross_wq, cross_qnorm,
                   cross_wo, cross_gates, cross_mlp_norm, cross_wgate, cross_wup, cross_wdown):
        kc = k_self.reshape(B, D, D)
        vc = v_self.reshape(B, D, D)
        cache = jax.ShapeDtypeStruct((B, D, D), BF16)
        kout, vout, q = pl.pallas_call(
            self_kernel,
            name='self_part',
            out_shape=(cache, cache, jax.ShapeDtypeStruct((B, HL, D), F32)),
            in_specs=[sm, vm] + [an] * 7,
            out_specs=(an, an, an),
            scratch_shapes=[VMEM((B, W), BF16), VMEM((B, W), BF16), VMEM((6, W, QC), BF16),
                            VMEM((B, D, D), BF16), VMEM((B, D, D), BF16),
                            VMEM((B, HL, D), F32), VMEM((2, B, D), F32), VMEM((2, B, D), F32),
                            VMEM((B, D), F32), VMEM((B, D), F32), VMEM((1, D), I32),
                            dma((6,)), dma((8,)), dma((8,)), dma((3,))],
            compiler_params=pltpu.CompilerParams(vmem_limit_bytes=MAXV),
        )(new_pos, self_attn_norm.reshape(R, D), new_pos[None, :], hidden, self_wq, self_wk, self_wv, kc, vc)

        part = VMEM((NG, R, HC), F32)
        parts3 = VMEM((3, NG, R, HC), F32)
        h4 = pl.pallas_call(
            rest_kernel,
            name='rest_part',
            out_shape=jax.ShapeDtypeStruct((B, W), BF16),
            in_specs=[sm, sm, sm, vm, vm, vm, vm] + [an] * 16,
            out_specs=vm,
            scratch_shapes=[
                VMEM((NP, 2, W, QC), BF16), VMEM((B, HL, D), F32), VMEM((NG, 2, HR + 1, HL, D), F32),
                VMEM((NG, 2, HR + 1, HL, D), F32),
                VMEM((R, W), F32), VMEM((R, W), BF16), VMEM((R, FF), BF16), VMEM((R, QW), BF16),
                VMEM((R, HL, D), F32), VMEM((NG, HR, D, D), BF16), VMEM((NG, HR, D, D), BF16),
                VMEM((R, D), I32), VMEM((R, D), F32),
                part, part, part, part,
                VMEM((4, NG, R, HC), F32), parts3, parts3,
                VMEM((NG, R, QC), F32), VMEM((NG, 2, 2, NG, R, QC), F32),
                dma((NP,)), dma((3,)), dma((2, NG)), dma((2, NG)), dma((2, NG)),
                dma((4, NG, 2)), dma((4, NG, 2)), dma((4, NG, 2)), dma((4, NG, 2)),
                dma((3, NG, 2)), dma((3, NG, 2)), dma((NG, NG)), dma((NG, NG)),
                dma((NG,)), dma((NG,)), dma((NG,)), dma((NG,))],
            compiler_params=pltpu.CompilerParams(collective_id=0, has_side_effects=True,
                                                 vmem_limit_bytes=MAXV),
        )(new_pos, rowmask, cross_gates, self_mlp_norm.reshape(R, D), cross_attn_norm.reshape(R, D),
          cross_mlp_norm.reshape(R, D), cross_qnorm[None, :], q, kout, vout, hidden, xvalid,
          k_cross.reshape(B, 2, D, D), v_cross.reshape(B, 2, D, D),
          self_wo, self_wgate, self_wup, self_wdown, cross_wq, cross_wo, cross_wgate, cross_wup, cross_wdown)
        return h4, kout.reshape(k_self.shape), vout.reshape(v_self.shape)

    return jax.shard_map(local_step, mesh=mesh, in_specs=in_specs, out_specs=out_specs, check_vma=False)
```

```python
import math
import jax
import jax.numpy as jnp
from jax import lax
from jax.experimental import pallas as pl
from jax.experimental.pallas import tpu as pltpu
from jax.sharding import PartitionSpec as P

NORM_EPS = 1e-5
ROPE_THETA = 500000.0
ROPE_FACTOR = 8.0
LOW_FREQ = 1.0
HIGH_FREQ = 4.0
ORIG_CTX = 8192.0
NEG_BIG = -1e30
F32 = jnp.float32
BF16 = jnp.bfloat16
I32 = jnp.int32
MESH = pl.DeviceIdType.MESH
ANY = pl.ANY
VMEM = pltpu.VMEM
SMEM = pltpu.SMEM
NP = 12
B = 128
R = 32
HR = 16
W = 4096
D = 128
HL = 8
QW = 1024
FF = 3072
SPAN = 64
NG = 4
HC = 512
QC = 256
SCALE = D ** -0.5
MAXV = 67043328
NT = (((1,), (1,)), ((), ()))
WIN = {'preferred_element_type': F32}
ORDER = (2, 3, 1, 0)
NEAR = (1, 3, 2)


def iota(shape, axis):
    return lax.broadcasted_iota(I32, shape, axis)


def rotary_freqs(lane):
    inv = jnp.exp((lane % SPAN).astype(F32) * (-2.0 / D * math.log(ROPE_THETA)))
    wave = 2.0 * math.pi / inv
    smooth = (ORIG_CTX / wave - LOW_FREQ) / (HIGH_FREQ - LOW_FREQ)
    mid = (1.0 - smooth) * inv / ROPE_FACTOR + smooth * inv
    scaled = jnp.where(wave > ORIG_CTX / LOW_FREQ, inv / ROPE_FACTOR, mid)
    return jnp.where(wave < ORIG_CTX / HIGH_FREQ, inv, scaled)


def norm_rows(src, gain, dst, r0, rows):
    at = slice(r0, r0 + rows)
    total = jnp.zeros((rows, D), F32)
    for c in range(0, W, D):
        v = src[at, c:c + D].astype(F32)
        total = total + v * v
    inv = lax.rsqrt(jnp.sum(total, axis=-1, keepdims=True) / W + NORM_EPS)
    for c in range(0, W, D):
        g = gain[c // D:c // D + 1, :].astype(F32)
        dst[at, c:c + D] = (src[at, c:c + D].astype(F32) * inv * g).astype(BF16)


def big_dot(lhs, rhs_of, depth, step=1024):
    acc = None
    for k in range(0, depth, step):
        part = jnp.dot(lhs[:, k:k + step], rhs_of(k, step), **WIN)
        acc = part if acc is None else acc + part
    return acc


def self_kernel(pos_s, g1, pos_a, hid, wq, wk, wv, kc, vc, kout, vout, qout,
                hb, xb, wb, kb, vb, q3, kn, vn, cs, sn, pv, w_sem, c_sem, o_sem, p_sem):
    base = lax.axis_index('sp') * SPAN

    def wcopy(i):
        src = (wk, wv)[i] if i < 2 else wq.at[:, (i - 2) * QC:(i - 1) * QC]
        return pltpu.make_async_copy(src, wb.at[i], w_sem.at[i])

    def ccopy(j):
        r = pl.ds((j // 2) * R, R)
        src, dst = ((kc, kb), (vc, vb))[j % 2]
        return pltpu.make_async_copy(src.at[r], dst.at[r], c_sem.at[j])

    def ocopy(j):
        r = pl.ds((j // 2) * R, R)
        src, dst = ((kb, kout), (vb, vout))[j % 2]
        return pltpu.make_async_copy(src.at[r], dst.at[r], o_sem.at[j])

    pcopy = pltpu.make_async_copy(pos_a, pv, p_sem.at[0])
    hcopy = pltpu.make_async_copy(hid, hb, p_sem.at[1])
    qcopy = pltpu.make_async_copy(q3, qout, p_sem.at[2])
    pcopy.start()
    hcopy.start()
    for i in range(2):
        wcopy(i).start(priority=1)
    for j in range(NG):
        wcopy(j + 2).start(priority=1)
        ccopy(2 * j).start(priority=1)
        ccopy(2 * j + 1).start(priority=1)

    pcopy.wait()
    ri = iota((B, D), 0)
    ci = iota((B, D), 1)
    posf = jnp.broadcast_to(pv[...].astype(F32), (B, D))
    pos_col = jnp.sum(jnp.where(ri == ci, posf, 0.0), axis=1, keepdims=True)
    ang = pos_col * jnp.broadcast_to(rotary_freqs(iota((1, D), 1)), (B, D))
    cs[...] = jnp.cos(ang)
    sn[...] = jnp.sin(ang) * jnp.where(ci < SPAN, -1.0, 1.0)

    hcopy.wait()
    norm_rows(hb, g1, xb, 0, B)

    def project(i):
        wcopy(i).wait()
        y = big_dot(xb, lambda k, w: wb[i, k:k + w, :], W).astype(BF16).astype(F32)
        for h in range(2):
            t = y[:, h * D:(h + 1) * D]
            if i != 1:
                t = t * cs[...] + pltpu.roll(t, SPAN, 1) * sn[...]
            t = t.astype(BF16).astype(F32)
            if i > 1:
                q3[:, (i - 2) * 2 + h, :] = t
            else:
                (kn, vn)[i][h] = t

    project(0)
    project(1)
    row16 = iota((HR, D), 0)
    for j in range(NG):
        project(j + 2)
        ccopy(2 * j).wait()
        ccopy(2 * j + 1).wait()

        def body(it, _):
            for u in range(HL):
                b = j * R + it * HL + u
                lp = pos_s[b] - base
                t0 = pl.multiple_of((jnp.clip(lp, 0, SPAN - 1) // HL) * HR, HR)
                hit = row16 + t0 - 2 * lp
                for buf, new in ((kb, kn), (vb, vn)):
                    old = buf[b, pl.ds(t0, HR), :].astype(F32)
                    upd = jnp.where(hit == 0, new[0, pl.ds(b, 1), :], jnp.where(hit == 1, new[1, pl.ds(b, 1), :], old))
                    buf[b, pl.ds(t0, HR), :] = upd.astype(BF16)
            return 0
        lax.fori_loop(0, R // HL, body, 0)
        ocopy(2 * j).start()
        ocopy(2 * j + 1).start()
    qcopy.start()
    for j in range(2 * NG):
        ocopy(j).wait()
    qcopy.wait()


def rest_kernel(pos_s, mask_s, gates, g2, g3, g4, qn, q_in, ks, vs, hid, xval, kc, vc,
                wo, wg1, wu1, wd1, wqc, woc, wg2, wu2, wd2, out,
                slots, qb, ob, orecv, h, x, act, o2, q3, kb, vb, xv, xl,
                p0, m0, s1, t1, rb1, rb2, rb3, rbq, fin, ov, v_sem,
                w_sem, m_sem, k_sem, sp_send, sp_recv, a_send, a_recv, y_send, y_recv,
                b_send, b_recv, z_send, z_recv, f_send, f_recv, e_send, e_recv):
    sp = lax.axis_index('sp')
    tp = lax.axis_index('tp')
    core = tp % 2
    ypos = tp // 2
    sib = {'tp': tp + 1 - 2 * core}
    ypeer = {'tp': (tp + 2) % 4}
    row0 = pl.multiple_of(sp * R, R)
    other = 1 - core
    turn = jnp.where(sp < 2, 1, -1)

    def half_col(g, half):
        return pl.multiple_of(g * 1024 + half * HC, HC)

    def remote(src, dst, ssem, rsem, dev):
        return pltpu.make_async_remote_copy(src, dst, ssem, rsem, device_id=dev, device_id_type=MESH)

    def cols(ref, c):
        return ref.at[:, pl.ds(pl.multiple_of(c, QC), QC)]

    def start(src, dst, slot):
        pltpu.make_async_copy(src, dst, w_sem.at[slot]).start(priority=1)

    def put_o(ref):
        def f(j, slot):
            for n in range(2):
                for k in range(4):
                    c = half_col(2 * j + n, other if k < 2 else core) + (k % 2) * QC
                    start(cols(ref, c), slots.at[slot, n, k * QW:(k + 1) * QW], slot)
        return f

    def put_gu(gate, up):
        def f(j, slot):
            start(cols(gate, j * QC), slots.at[slot, 0], slot)
            start(cols(up, j * QC), slots.at[slot, 1], slot)
        return f

    def put_down(ref):
        def f(j, slot):
            part = j % 2
            c = half_col(j // 2, other + part * (core - other))
            for n in range(2):
                start(cols(ref, c + n * QC), slots.at[slot, n, 0:FF], slot)
        return f

    def put_q(ref):
        def f(j, slot):
            for n in range(2):
                start(cols(ref, (2 * j + n) * QC), slots.at[slot, n], slot)
        return f

    puts = (put_o(wo), put_gu(wg1, wu1), put_down(wd1), put_q(wqc), put_o(woc), put_gu(wg2, wu2), put_down(wd2))
    starts = [0]
    for count in (2, 12, 8, 2, 2, 12, 8):
        starts.append(starts[-1] + count)
    last_pair = starts.pop()

    def slot_of(seg, j):
        p = starts[seg] % NP + j
        if isinstance(p, int):
            return p % NP
        return jnp.where(p >= NP, p - NP, p)

    def wait_pair(seg, j, depth=W):
        slot = slot_of(seg, j)
        dst = slots.at[slot] if depth == W else slots.at[slot, :, 0:depth]
        pltpu.make_async_copy(dst, dst, w_sem.at[slot]).wait()
        return slot

    def refill(seg, j, first):
        p = starts[seg] + first + NP
        if p < last_pair:
            to = max(n for n in range(len(starts)) if starts[n] <= p)
            puts[to](j + (starts[seg] + NP - starts[to]), slot_of(seg, j))

    def sub_loops(seg, body):
        count = {1: 12, 5: 12}[seg]
        edges = sorted({0, count} | {e - NP - starts[seg] for e in starts + [last_pair] if 0 < e - NP - starts[seg] < count})
        for a, b in zip(edges, edges[1:]):
            def run(j, c, a=a):
                body(j, a)
                return c
            lax.fori_loop(a, b, run, 0)

    def dest_of(n):
        return (sp + turn * ORDER[n % NG] + NG) % NG

    def kv_self(n):
        r = pl.ds(pl.multiple_of(dest_of(n) * R + (n // NG) * HR, HR), HR)
        return [pltpu.make_async_copy(src.at[r], dst.at[n % NG], k_sem.at[i, n % NG])
                for i, (src, dst) in enumerate(((ks, kb), (vs, vb)))]

    def kv_cross(n):
        r = pl.ds(pl.multiple_of(row0 + (n // 2) * HR, HR), HR)
        return [pltpu.make_async_copy(src.at[r, n % 2], dst.at[n], k_sem.at[i, n])
                for i, (src, dst) in enumerate(((kc, kb), (vc, vb)))]

    def go(cs):
        for c in cs:
            c.start()

    def fin_wait(cs):
        for c in cs:
            c.wait()

    qcopy = pltpu.make_async_copy(q_in, qb, m_sem.at[0])
    hcopy = pltpu.make_async_copy(hid.at[pl.ds(row0, R)], x, m_sem.at[1])
    xcopy = pltpu.make_async_copy(xval.at[pl.ds(row0, R)], xv, m_sem.at[2])
    go([qcopy])
    for n in range(NG):
        go(kv_self(n))
    go([hcopy, xcopy])

    for j in range(2):
        puts[0](j, slot_of(0, j))

    def fill(j, _):
        puts[1](j, slot_of(1, j))
        return 0
    lax.fori_loop(0, NP - 2, fill, 0)

    barrier = pltpu.get_barrier_semaphore()
    for dev in [{'sp': (sp + d) % NG} for d in ORDER[:3]] + [sib, ypeer]:
        pl.semaphore_signal(barrier, inc=1, device_id=dev, device_id_type=MESH)
    pl.semaphore_wait(barrier, 5)

    lane = iota((HL, D), 1)
    par = (lane % 2) == (iota((HL, D), 0) // 4)

    def scores(q, k):
        return lax.dot_general(q.astype(BF16), k, NT, **WIN) * SCALE

    def sp_copy(n):
        d = ORDER[n % NG]
        half = n // NG
        return remote(ob.at[d, half], orecv.at[sp, half], sp_send.at[0], sp_recv.at[half, sp],
                      {'sp': dest_of(n)})

    def sp_arrival(half, d):
        src = (sp + d) % NG
        return remote(ob.at[d, half], orecv.at[src, half], sp_send.at[0], sp_recv.at[half, src], {'sp': src})

    def attend_stage(n):
        half = n // NG
        d = ORDER[n % NG]
        fin_wait(kv_self(n))
        first = dest_of(n) * R + half * HR
        slot = n % NG

        def body(it, st):
            res = []
            for u in range(HL):
                v = it * HL + u
                lp = pos_s[first + v] - sp * SPAN
                s = scores(qb[first + v], kb[slot, v])
                ok = par & (lane <= 2 * lp + 1)
                s = jnp.where(ok, s, NEG_BIG)
                m = jnp.max(s, axis=-1, keepdims=True)
                p = jnp.where(ok, jnp.exp(s - m), 0.0)
                res.append((m, jnp.sum(p, axis=-1, keepdims=True), p))
            for u in range(HL):
                v = it * HL + u
                m, l, p = res[u]
                o = jnp.dot(p.astype(BF16), vb[slot, v], **WIN)
                if d:
                    ob[d, half, v] = o
                else:
                    orecv[sp, half, v] = o
                st = jnp.where(lane == v, m, jnp.where(lane == HR + v, l, st))
            return st
        st = lax.fori_loop(0, HR // HL, body, jnp.zeros((HL, D), F32))
        if d:
            ob[d, half, HR] = st
            sp_copy(n).start()
        else:
            orecv[sp, half, HR] = st

    def combine(half):
        for d in ORDER[:3]:
            sp_arrival(half, d).wait_recv()
        st = [orecv[s, half, HR] for s in range(NG)]
        gm = jnp.maximum(jnp.maximum(st[0], st[1]), jnp.maximum(st[2], st[3]))
        fac = [jnp.exp(v - gm) for v in st]
        tot = jnp.zeros((HL, D), F32)
        for v, f in zip(st, fac):
            tot = tot + pltpu.roll(v, D - HR, 1) * f
        wts = [f / tot for f in fac]
        for r in range(HR):
            acc = jnp.zeros((HL, D), F32)
            for s in range(NG):
                acc = acc + orecv[s, half, r] * wts[s][:, r:r + 1]
            q3[half * HR + r] = acc
        flatten(half)

    def flatten(half):
        at = slice(half * HR, half * HR + HR)
        for hh in range(HL):
            o2[at, hh * D:(hh + 1) * D] = q3[at, hh, :].astype(BF16)

    def d2d(k, g, half):
        at = pl.ds(half * HR, HR)
        return remote(p0.at[g, at], rb1.at[k, g, at], a_send.at[0], a_recv.at[k % 2, g, half], sib)

    def ycp(k, g, half):
        at = pl.ds(half * HR, HR)
        return remote(s1.at[g, at], rb2.at[k, g, at], y_send.at[0], y_recv.at[k % 2, g, half], ypeer)

    def back(k, g, half):
        at = pl.ds(half * HR, HR)
        return remote(t1.at[g, at], rb3.at[k, g, at], b_send.at[0], b_recv.at[k % 2, g, half], sib)

    def add_core(k, g, half):
        at = slice(half * HR, half * HR + HR)
        d2d(k, g, half).wait_recv()
        s1[g, at] = m0[g, at] + rb1[k, g, at]
        ycp(k, g, half).start()

    def add_chip(k, g, half):
        at = slice(half * HR, half * HR + HR)
        ycp(k, g, half).wait_recv()
        t1[g, at] = s1[g, at] + rb2[k, g, at]
        back(k, g, half).start()

    def settle(k, half, scale_col):
        at = slice(half * HR, half * HR + HR)

        def upd(src, c0):
            to = pl.ds(c0, HC)
            v = src if scale_col is None else scale_col[at] * src
            h[at, to] = (h[at, to] + v).astype(BF16).astype(F32)
        for g in range(NG):
            upd(t1[g, at], half_col(g, core))
        for g in range(NG):
            back(k, g, half).wait_recv()
            upd(rb3[k, g, at], half_col(g, other))

    def sent(ref, sem):
        pltpu.make_async_copy(ref, ref, sem.at[0]).wait()

    def drain(k):
        for ref, sem in ((p0, a_send), (s1, y_send), (t1, b_send)):
            sent(ref, sem)

    def o_products(k, seg, half, last):
        at = slice(half * HR, half * HR + HR)
        for g in range(NG):
            slot = slot_of(seg, g // 2)
            if half == 0 and g % 2 == 0:
                wait_pair(seg, g // 2)
            r = [jnp.dot(o2[at, :], slots[slot, g % 2, n * QW:(n + 1) * QW, :], **WIN) for n in range(4)]
            p0[g, at] = jnp.concatenate(r[:2], axis=1)
            d2d(k, g, half).start()
            m0[g, at] = jnp.concatenate(r[2:], axis=1)
            if last and g % 2:
                refill(seg, g // 2, g // 2)

    def down_product(seg):
        def f(g, part):
            j = 2 * g + part
            slot = wait_pair(seg, j, FF)
            r = [big_dot(act, lambda k, w: slots[slot, n, pl.ds(k, w), :], FF) for n in range(2)]
            refill(seg, j, 0)
            return jnp.concatenate(r, axis=1)
        return f

    def reduce_down(k, seg):
        product = down_product(seg)

        def both(g):
            for half in range(2):
                add_core(k, g, half)

        def body(g, _):
            p0[g] = product(g, 0)
            for half in range(2):
                d2d(k, g, half).start()

            @pl.when(g > 0)
            def _():
                both(g - 1)
            m0[g] = product(g, 1)
            return 0
        lax.fori_loop(0, NG, body, 0)
        both(3)

    def gate_up(seg, gain):
        for half in range(2):
            norm_rows(h, gain, x, half * HR, HR)

        def body(j, first):
            slot = wait_pair(seg, j)
            gv, uv = [big_dot(x, lambda k, w: slots[slot, n, pl.ds(k, w), :], W).astype(BF16).astype(F32) for n in range(2)]
            refill(seg, j, first)
            act[:, pl.ds(pl.multiple_of(j * QC, QC), QC)] = (gv * (1.0 / (1.0 + jnp.exp(-gv))) * uv).astype(BF16)
        sub_loops(seg, body)

    rid = iota((R, D), 0)
    maskv = jnp.zeros((R, D), F32)
    for r in range(R):
        maskv = jnp.where(rid == r, mask_s[row0 + r].astype(F32), maskv)
    mask_col = maskv[:, 0:1]

    fin_wait([qcopy])
    for n in range(2 * NG):
        attend_stage(n)
        if n < NG:
            go(kv_self(n + NG))
        else:
            go(kv_cross(n - NG))
    fin_wait([hcopy])
    for c in range(0, W, HC):
        h[:, c:c + HC] = x[:, c:c + HC].astype(F32)

    def groups(f, k, half):
        for g in range(NG):
            f(k, g, half)

    combine(0)
    o_products(0, 0, 0, False)
    groups(add_core, 0, 0)
    combine(1)
    o_products(0, 0, 1, True)
    groups(add_core, 0, 1)
    groups(add_chip, 0, 0)
    settle(0, 0, None)
    groups(add_chip, 0, 1)
    settle(0, 1, None)
    drain(0)
    gate_up(1, g2)

    reduce_down(1, 2)
    for half in range(2):
        groups(add_chip, 1, half)
    for half in range(2):
        settle(1, half, None)
    drain(1)

    for half in range(2):
        norm_rows(h, g3, x, half * HR, HR)
    for j in range(2):
        slot = wait_pair(3, j)
        ys = [big_dot(x, lambda k, w: slots[slot, n, pl.ds(k, w), :], W).astype(BF16).astype(F32) for n in range(2)]
        refill(3, j, j)
        for hh in range(4):
            t = ys[hh // 2][:, hh % 2 * D:(hh % 2 + 1) * D]
            inv = lax.rsqrt(jnp.mean(t * t, axis=-1, keepdims=True) + NORM_EPS)
            q3[:, NG * j + hh, :] = (t * inv * qn[...].astype(F32)).astype(BF16).astype(F32)
    fin_wait([xcopy])
    xlen = jnp.sum(jnp.where(xv[...] > 0, 1.0, 0.0), axis=-1, keepdims=True)
    xl[...] = jnp.broadcast_to(2.0 * xlen, (R, D))
    lane2 = iota((HL, 2 * D), 1)
    par2 = (lane2 % 2) == (iota((HL, 2 * D), 0) // 4)
    lanef = lane2.astype(F32)

    for half in range(2):
        fin_wait(kv_cross(2 * half) + kv_cross(2 * half + 1))

        def xbody(it, _):
            res = []
            for u in range(HL):
                v = it * HL + u
                b = half * HR + v
                s = jnp.concatenate([scores(q3[b], kb[2 * half + t, v]) for t in range(2)], axis=1)
                ok = par2 & (lanef < xl[pl.ds(b, 1), :][:, 0:1])
                s = jnp.where(ok, s, NEG_BIG)
                m = jnp.max(s, axis=-1, keepdims=True)
                p = jnp.where(ok, jnp.exp(s - m), 0.0)
                res.append((p, jnp.sum(p, axis=-1, keepdims=True)))
            for u in range(HL):
                v = it * HL + u
                p, l = res[u]
                o = sum(jnp.dot(p[:, t * D:(t + 1) * D].astype(BF16), vb[2 * half + t, v], **WIN) for t in range(2))
                q3[half * HR + v] = o / l
            return 0
        lax.fori_loop(0, HR // HL, xbody, 0)
        flatten(half)

    ga = jnp.tanh(jnp.full((R, 1), gates[0], F32)) * mask_col
    gm2 = jnp.tanh(jnp.full((R, 1), gates[1], F32)) * mask_col
    for half in range(2):
        o_products(2, 4, half, half == 1)
        groups(add_core, 2, half)
    for half in range(2):
        groups(add_chip, 2, half)
    for half in range(2):
        settle(2, half, ga)
    drain(2)
    gate_up(5, g4)

    product = down_product(6)

    def quarter(y):
        return pl.ds(pl.multiple_of(y * QC, QC), QC)

    def last_d2d(g):
        return remote(p0.at[g], rb1.at[3, g], a_send.at[0], a_recv.at[1, g, 0], sib)

    def qcp(g):
        return remote(s1.at[g, :, quarter(1 - ypos)], rbq.at[g], y_send.at[0], y_recv.at[1, g, 0], ypeer)

    def zcp(g, d):
        piece = fin.at[g, core, ypos, sp]
        return remote(piece, piece, z_send.at[0], z_recv.at[g, d], {'sp': (sp + d) % NG})

    def fcp(g, d):
        z = (sp + NG - d) % NG
        piece = fin.at[g, core, ypos, z]
        return remote(piece, piece, f_send.at[0], f_recv.at[g, d], ypeer)

    def ecp(g):
        piece = fin.at[g, core]
        return remote(piece, piece, e_send.at[0], e_recv.at[g], sib)

    def stage_q(g):
        qcp(g).wait_recv()
        c0 = pl.multiple_of(half_col(g, core) + ypos * QC, QC)
        t = s1[g, :, quarter(ypos)] + rbq[g]
        fin[g, core, ypos, sp] = (h[:, pl.ds(c0, QC)] + gm2 * t).astype(BF16).astype(F32)
        for d in NEAR:
            zcp(g, d).start()
        fcp(g, 0).start()

    def stage_f(g):
        for d in NEAR:
            zcp(g, d).wait_recv()
            fcp(g, d).start()

    def stage_e(g):
        for d in (0,) + NEAR:
            fcp(g, d).wait_recv()
        ecp(g).start()

    def stage_c(g):
        last_d2d(g).wait_recv()
        s1[g] = m0[g] + rb1[3, g]
        qcp(g).start()

    def body(g, _):
        p0[g] = product(g, 0)
        last_d2d(g).start()

        @pl.when(g > 0)
        def _():
            stage_c(g - 1)
        m0[g] = product(g, 1)

        @pl.when(g > 1)
        def _():
            stage_q(g - 2)
        return 0
    lax.fori_loop(0, NG, body, 0)
    stage_c(3)
    stage_q(2)
    stage_q(3)
    stage_f(0)
    stage_f(1)
    stage_e(0)
    stage_f(2)
    stage_e(1)
    stage_f(3)
    stage_e(2)
    stage_e(3)

    def emit(g, half):
        for yy in range(2):
            c = pl.multiple_of(half_col(g, half) + yy * QC, QC)
            for zz in range(NG):
                ov[zz * R:(zz + 1) * R, pl.ds(c, QC)] = fin[g, half, yy, zz].astype(BF16)

    def out_copy(g, n):
        at = pl.ds(half_col(g, (core, other)[n]), HC)
        return pltpu.make_async_copy(ov.at[:, at], out.at[:, at], v_sem.at[0])

    for g in range(NG):
        emit(g, core)
        out_copy(g, 0).start()
    for g in range(NG):
        ecp(g).wait_recv()
        emit(g, other)
        out_copy(g, 1).start()
    pltpu.make_async_copy(ov, out, v_sem.at[0]).wait()
    sent(ob.at[1:NG], sp_send)
    sent(p0, a_send)
    sent(s1.at[:, :, 0:QC], y_send)
    sent(fin.at[0:3, 0, 0], z_send)
    sent(fin.at[:, 0, 0], f_send)
    sent(fin.at[:, 0], e_send)


def solution(mesh):
    cache_spec = P('dp', 'sp', 'tp', None)
    cross_spec = P('dp', None, 'tp', None)
    row_spec = P('dp', None)
    vec_spec = P('dp')
    full_spec = P(None)
    col_spec = P(None, 'tp')
    split_rows = P('tp', None)
    in_specs = (row_spec, vec_spec, cache_spec, cache_spec, cross_spec, cross_spec, row_spec, vec_spec,
                full_spec, col_spec, col_spec, col_spec, split_rows, full_spec, col_spec, col_spec, split_rows,
                full_spec, col_spec, full_spec, split_rows, full_spec, full_spec, col_spec, col_spec, split_rows)
    out_specs = (row_spec, cache_spec, cache_spec)
    vm = pl.BlockSpec(memory_space=VMEM)
    sm = pl.BlockSpec(memory_space=SMEM)
    an = pl.BlockSpec(memory_space=ANY)
    dma = pltpu.SemaphoreType.DMA

    def local_step(hidden, new_pos, k_self, v_self, k_cross, v_cross, xvalid, rowmask,
                   self_attn_norm, self_wq, self_wk, self_wv, self_wo, self_mlp_norm,
                   self_wgate, self_wup, self_wdown, cross_attn_norm, cross_wq, cross_qnorm,
                   cross_wo, cross_gates, cross_mlp_norm, cross_wgate, cross_wup, cross_wdown):
        kc = k_self.reshape(B, D, D)
        vc = v_self.reshape(B, D, D)
        cache = jax.ShapeDtypeStruct((B, D, D), BF16)
        kout, vout, q = pl.pallas_call(
            self_kernel,
            name='self_part',
            out_shape=(cache, cache, jax.ShapeDtypeStruct((B, HL, D), F32)),
            in_specs=[sm, vm] + [an] * 7,
            out_specs=(an, an, an),
            scratch_shapes=[VMEM((B, W), BF16), VMEM((B, W), BF16), VMEM((6, W, QC), BF16),
                            VMEM((B, D, D), BF16), VMEM((B, D, D), BF16),
                            VMEM((B, HL, D), F32), VMEM((2, B, D), F32), VMEM((2, B, D), F32),
                            VMEM((B, D), F32), VMEM((B, D), F32), VMEM((1, D), I32),
                            dma((6,)), dma((8,)), dma((8,)), dma((3,))],
            compiler_params=pltpu.CompilerParams(vmem_limit_bytes=MAXV),
        )(new_pos, self_attn_norm.reshape(R, D), new_pos[None, :], hidden, self_wq, self_wk, self_wv, kc, vc)

        part = VMEM((NG, R, HC), F32)
        parts3 = VMEM((3, NG, R, HC), F32)
        h4 = pl.pallas_call(
            rest_kernel,
            name='rest_part',
            out_shape=jax.ShapeDtypeStruct((B, W), BF16),
            in_specs=[sm, sm, sm, vm, vm, vm, vm] + [an] * 16,
            out_specs=an,
            scratch_shapes=[
                VMEM((NP, 2, W, QC), BF16), VMEM((B, HL, D), F32), VMEM((NG, 2, HR + 1, HL, D), F32),
                VMEM((NG, 2, HR + 1, HL, D), F32),
                VMEM((R, W), F32), VMEM((R, W), BF16), VMEM((R, FF), BF16), VMEM((R, QW), BF16),
                VMEM((R, HL, D), F32), VMEM((NG, HR, D, D), BF16), VMEM((NG, HR, D, D), BF16),
                VMEM((R, D), I32), VMEM((R, D), F32),
                part, part, part, part,
                VMEM((4, NG, R, HC), F32), parts3, parts3,
                VMEM((NG, R, QC), F32), VMEM((NG, 2, 2, NG, R, QC), F32), VMEM((B, W), BF16), dma((1,)),
                dma((NP,)), dma((3,)), dma((2, NG)), dma((1,)), dma((2, NG)),
                dma((1,)), dma((2, NG, 2)), dma((1,)), dma((2, NG, 2)), dma((1,)), dma((2, NG, 2)),
                dma((1,)), dma((NG, NG)), dma((1,)), dma((NG, NG)), dma((1,)), dma((NG,))],
            compiler_params=pltpu.CompilerParams(collective_id=0, has_side_effects=True,
                                                 vmem_limit_bytes=MAXV),
        )(new_pos, rowmask, cross_gates, self_mlp_norm.reshape(R, D), cross_attn_norm.reshape(R, D),
          cross_mlp_norm.reshape(R, D), cross_qnorm[None, :], q, kout, vout, hidden, xvalid,
          k_cross.reshape(B, 2, D, D), v_cross.reshape(B, 2, D, D),
          self_wo, self_wgate, self_wup, self_wdown, cross_wq, cross_wo, cross_wgate, cross_wup, cross_wdown)
        return h4, kout.reshape(k_self.shape), vout.reshape(v_self.shape)

    return jax.shard_map(local_step, mesh=mesh, in_specs=in_specs, out_specs=out_specs, check_vma=False)
```

```python
import math
import jax
import jax.numpy as jnp
from jax import lax
from jax.experimental import pallas as pl
from jax.experimental.pallas import tpu as pltpu
from jax.sharding import PartitionSpec as P

NORM_EPS = 1e-5
ROPE_THETA = 500000.0
ROPE_FACTOR = 8.0
LOW_FREQ = 1.0
HIGH_FREQ = 4.0
ORIG_CTX = 8192.0
NEG_BIG = -1e30
F32 = jnp.float32
BF16 = jnp.bfloat16
I32 = jnp.int32
MESH = pl.DeviceIdType.MESH
ANY = pl.ANY
VMEM = pltpu.VMEM
SMEM = pltpu.SMEM
NP = 12
B = 128
R = 32
HR = 16
W = 4096
D = 128
HL = 8
QW = 1024
FF = 3072
SPAN = 64
NG = 4
HC = 512
QC = 256
SCALE = D ** -0.5
MAXV = 67043328
NT = (((1,), (1,)), ((), ()))
WIN = {'preferred_element_type': F32}
ORDER = (2, 3, 1, 0)
NEAR = (1, 3, 2)


def iota(shape, axis):
    return lax.broadcasted_iota(I32, shape, axis)


def rotary_freqs(lane):
    inv = jnp.exp((lane % SPAN).astype(F32) * (-2.0 / D * math.log(ROPE_THETA)))
    wave = 2.0 * math.pi / inv
    smooth = (ORIG_CTX / wave - LOW_FREQ) / (HIGH_FREQ - LOW_FREQ)
    mid = (1.0 - smooth) * inv / ROPE_FACTOR + smooth * inv
    scaled = jnp.where(wave > ORIG_CTX / LOW_FREQ, inv / ROPE_FACTOR, mid)
    return jnp.where(wave < ORIG_CTX / HIGH_FREQ, inv, scaled)


def norm_rows(src, gain, dst, r0, rows):
    at = slice(r0, r0 + rows)
    total = jnp.zeros((rows, D), F32)
    for c in range(0, W, D):
        v = src[at, c:c + D].astype(F32)
        total = total + v * v
    inv = lax.rsqrt(jnp.sum(total, axis=-1, keepdims=True) / W + NORM_EPS)
    for c in range(0, W, D):
        g = gain[c // D:c // D + 1, :].astype(F32)
        dst[at, c:c + D] = (src[at, c:c + D].astype(F32) * inv * g).astype(BF16)


def big_dot(lhs, rhs_of, depth, step=1024):
    acc = None
    for k in range(0, depth, step):
        part = jnp.dot(lhs[:, k:k + step], rhs_of(k, step), **WIN)
        acc = part if acc is None else acc + part
    return acc


def self_kernel(pos_s, g1, pos_a, hid, wq, wk, wv, kc, vc, kout, vout, qout,
                hb, xb, wb, kb, vb, q3, kn, vn, cs, sn, pv, w_sem, c_sem, o_sem, p_sem):
    base = lax.axis_index('sp') * SPAN

    def wcopy(i):
        src = (wk, wv)[i] if i < 2 else wq.at[:, (i - 2) * QC:(i - 1) * QC]
        return pltpu.make_async_copy(src, wb.at[i], w_sem.at[i])

    def ccopy(j):
        r = pl.ds((j // 2) * R, R)
        src, dst = ((kc, kb), (vc, vb))[j % 2]
        return pltpu.make_async_copy(src.at[r], dst.at[r], c_sem.at[j])

    def ocopy(j):
        r = pl.ds((j // 2) * R, R)
        src, dst = ((kb, kout), (vb, vout))[j % 2]
        return pltpu.make_async_copy(src.at[r], dst.at[r], o_sem.at[j])

    pcopy = pltpu.make_async_copy(pos_a, pv, p_sem.at[0])
    hcopy = pltpu.make_async_copy(hid, hb, p_sem.at[1])
    qcopy = pltpu.make_async_copy(q3, qout, p_sem.at[2])
    pcopy.start()
    hcopy.start()
    for i in range(2):
        wcopy(i).start(priority=1)
    for j in range(NG):
        wcopy(j + 2).start(priority=1)
        ccopy(2 * j).start(priority=1)
        ccopy(2 * j + 1).start(priority=1)

    pcopy.wait()
    ri = iota((B, D), 0)
    ci = iota((B, D), 1)
    posf = jnp.broadcast_to(pv[...].astype(F32), (B, D))
    pos_col = jnp.sum(jnp.where(ri == ci, posf, 0.0), axis=1, keepdims=True)
    ang = pos_col * jnp.broadcast_to(rotary_freqs(iota((1, D), 1)), (B, D))
    cs[...] = jnp.cos(ang)
    sn[...] = jnp.sin(ang) * jnp.where(ci < SPAN, -1.0, 1.0)

    hcopy.wait()
    norm_rows(hb, g1, xb, 0, B)

    def project(i):
        wcopy(i).wait()
        y = big_dot(xb, lambda k, w: wb[i, k:k + w, :], W).astype(BF16).astype(F32)
        for h in range(2):
            t = y[:, h * D:(h + 1) * D]
            if i != 1:
                t = t * cs[...] + pltpu.roll(t, SPAN, 1) * sn[...]
            t = t.astype(BF16).astype(F32)
            if i > 1:
                q3[:, (i - 2) * 2 + h, :] = t
            else:
                (kn, vn)[i][h] = t

    project(0)
    project(1)
    row16 = iota((HR, D), 0)
    for j in range(NG):
        project(j + 2)
        ccopy(2 * j).wait()
        ccopy(2 * j + 1).wait()

        def body(it, _):
            for u in range(HL):
                b = j * R + it * HL + u
                lp = pos_s[b] - base
                t0 = pl.multiple_of((jnp.clip(lp, 0, SPAN - 1) // HL) * HR, HR)
                hit = row16 + t0 - 2 * lp
                for buf, new in ((kb, kn), (vb, vn)):
                    old = buf[b, pl.ds(t0, HR), :].astype(F32)
                    upd = jnp.where(hit == 0, new[0, pl.ds(b, 1), :], jnp.where(hit == 1, new[1, pl.ds(b, 1), :], old))
                    buf[b, pl.ds(t0, HR), :] = upd.astype(BF16)
            return 0
        lax.fori_loop(0, R // HL, body, 0)
        ocopy(2 * j).start()
        ocopy(2 * j + 1).start()
    qcopy.start()
    for j in range(2 * NG):
        ocopy(j).wait()
    qcopy.wait()


def rest_kernel(pos_s, mask_s, gates, g2, g3, g4, qn, q_in, ks, vs, hid, xval, kc, vc,
                wo, wg1, wu1, wd1, wqc, woc, wg2, wu2, wd2, out,
                slots, qb, ob, orecv, h, x, act, o2, q3, kb, vb, xv, xl,
                p0, m0, s1, t1, rb1, rb2, rb3, rbq, fin, ov, v_sem, q_sem,
                w_sem, m_sem, k_sem, sp_send, sp_recv, a_send, a_recv, y_send, y_recv,
                b_send, b_recv, z_send, z_recv, f_send, f_recv, e_send, e_recv):
    sp = lax.axis_index('sp')
    tp = lax.axis_index('tp')
    core = tp % 2
    ypos = tp // 2
    sib = {'tp': tp + 1 - 2 * core}
    ypeer = {'tp': (tp + 2) % 4}
    row0 = pl.multiple_of(sp * R, R)
    other = 1 - core
    turn = jnp.where(sp < 2, 1, -1)

    def half_col(g, half):
        return pl.multiple_of(g * 1024 + half * HC, HC)

    def remote(src, dst, ssem, rsem, dev):
        return pltpu.make_async_remote_copy(src, dst, ssem, rsem, device_id=dev, device_id_type=MESH)

    def cols(ref, c):
        return ref.at[:, pl.ds(pl.multiple_of(c, QC), QC)]

    def start(src, dst, slot):
        pltpu.make_async_copy(src, dst, w_sem.at[slot]).start(priority=1)

    def put_o(ref):
        def f(j, slot):
            for n in range(2):
                for k in range(4):
                    c = half_col(2 * j + n, other if k < 2 else core) + (k % 2) * QC
                    start(cols(ref, c), slots.at[slot, n, k * QW:(k + 1) * QW], slot)
        return f

    def put_gu(gate, up):
        def f(j, slot):
            start(cols(gate, j * QC), slots.at[slot, 0], slot)
            start(cols(up, j * QC), slots.at[slot, 1], slot)
        return f

    def put_down(ref):
        def f(j, slot):
            part = j % 2
            c = half_col(j // 2, other + part * (core - other))
            for n in range(2):
                start(cols(ref, c + n * QC), slots.at[slot, n, 0:FF], slot)
        return f

    def put_q(ref):
        def f(j, slot):
            for n in range(2):
                start(cols(ref, (2 * j + n) * QC), slots.at[slot, n], slot)
        return f

    puts = (put_o(wo), put_gu(wg1, wu1), put_down(wd1), put_q(wqc), put_o(woc), put_gu(wg2, wu2), put_down(wd2))
    starts = [0]
    for count in (2, 12, 8, 2, 2, 12, 8):
        starts.append(starts[-1] + count)
    last_pair = starts.pop()

    def slot_of(seg, j):
        p = starts[seg] % NP + j
        if isinstance(p, int):
            return p % NP
        return jnp.where(p >= NP, p - NP, p)

    def wait_pair(seg, j, depth=W):
        slot = slot_of(seg, j)
        dst = slots.at[slot] if depth == W else slots.at[slot, :, 0:depth]
        pltpu.make_async_copy(dst, dst, w_sem.at[slot]).wait()
        return slot

    def refill(seg, j, first):
        p = starts[seg] + first + NP
        if p < last_pair:
            to = max(n for n in range(len(starts)) if starts[n] <= p)
            puts[to](j + (starts[seg] + NP - starts[to]), slot_of(seg, j))

    def sub_loops(seg, body):
        count = {1: 12, 5: 12}[seg]
        edges = sorted({0, count} | {e - NP - starts[seg] for e in starts + [last_pair] if 0 < e - NP - starts[seg] < count})
        for a, b in zip(edges, edges[1:]):
            def run(j, c, a=a):
                body(j, a)
                return c
            lax.fori_loop(a, b, run, 0)

    def dest_of(n):
        return (sp + turn * ORDER[n % NG] + NG) % NG

    def kv_self(n):
        r = pl.ds(pl.multiple_of(dest_of(n) * R + (n // NG) * HR, HR), HR)
        return [pltpu.make_async_copy(src.at[r], dst.at[n % NG], k_sem.at[i, n % NG])
                for i, (src, dst) in enumerate(((ks, kb), (vs, vb)))]

    def kv_cross(n):
        r = pl.ds(pl.multiple_of(row0 + (n // 2) * HR, HR), HR)
        return [pltpu.make_async_copy(src.at[r, n % 2], dst.at[n], k_sem.at[i, n])
                for i, (src, dst) in enumerate(((kc, kb), (vc, vb)))]

    def go(cs):
        for c in cs:
            c.start()

    def fin_wait(cs):
        for c in cs:
            c.wait()

    def qcopy(n):
        r = pl.ds(pl.multiple_of(dest_of(n) * R + (n // NG) * HR, HR), HR)
        return pltpu.make_async_copy(q_in.at[r], qb.at[r], q_sem.at[n])

    hcopy = pltpu.make_async_copy(hid.at[pl.ds(row0, R)], x, m_sem.at[1])
    xcopy = pltpu.make_async_copy(xval.at[pl.ds(row0, R)], xv, m_sem.at[2])
    for n in range(NG):
        go([qcopy(n)] + kv_self(n))
    go([qcopy(n) for n in range(NG, 2 * NG)])
    go([hcopy, xcopy])

    for j in range(2):
        puts[0](j, slot_of(0, j))

    def fill(j, _):
        puts[1](j, slot_of(1, j))
        return 0
    lax.fori_loop(0, NP - 2, fill, 0)

    barrier = pltpu.get_barrier_semaphore()
    for dev in [{'sp': (sp + d) % NG} for d in ORDER[:3]] + [sib, ypeer]:
        pl.semaphore_signal(barrier, inc=1, device_id=dev, device_id_type=MESH)

    lane = iota((HL, D), 1)
    par = (lane % 2) == (iota((HL, D), 0) // 4)

    def scores(q, k):
        return lax.dot_general(q.astype(BF16), k, NT, **WIN) * SCALE

    def sp_copy(n):
        d = ORDER[n % NG]
        half = n // NG
        return remote(ob.at[d, half], orecv.at[sp, half], sp_send.at[0], sp_recv.at[half, sp],
                      {'sp': dest_of(n)})

    def sp_arrival(half, d):
        src = (sp + d) % NG
        return remote(ob.at[d, half], orecv.at[src, half], sp_send.at[0], sp_recv.at[half, src], {'sp': src})

    def attend_stage(n):
        half = n // NG
        d = ORDER[n % NG]
        fin_wait([qcopy(n)] + kv_self(n))
        first = dest_of(n) * R + half * HR
        slot = n % NG

        def body(it, st):
            res = []
            for u in range(HL):
                v = it * HL + u
                lp = pos_s[first + v] - sp * SPAN
                s = scores(qb[first + v], kb[slot, v])
                ok = par & (lane <= 2 * lp + 1)
                s = jnp.where(ok, s, NEG_BIG)
                m = jnp.max(s, axis=-1, keepdims=True)
                p = jnp.where(ok, jnp.exp(s - m), 0.0)
                res.append((m, jnp.sum(p, axis=-1, keepdims=True), p))
            for u in range(HL):
                v = it * HL + u
                m, l, p = res[u]
                o = jnp.dot(p.astype(BF16), vb[slot, v], **WIN)
                if d:
                    ob[d, half, v] = o
                else:
                    orecv[sp, half, v] = o
                st = jnp.where(lane == v, m, jnp.where(lane == HR + v, l, st))
            return st
        st = lax.fori_loop(0, HR // HL, body, jnp.zeros((HL, D), F32))
        if d:
            ob[d, half, HR] = st
            if n == 0:
                pl.semaphore_wait(barrier, 5)
            sp_copy(n).start()
        else:
            orecv[sp, half, HR] = st

    def combine(half):
        for d in ORDER[:3]:
            sp_arrival(half, d).wait_recv()
        st = [orecv[s, half, HR] for s in range(NG)]
        gm = jnp.maximum(jnp.maximum(st[0], st[1]), jnp.maximum(st[2], st[3]))
        fac = [jnp.exp(v - gm) for v in st]
        tot = jnp.zeros((HL, D), F32)
        for v, f in zip(st, fac):
            tot = tot + pltpu.roll(v, D - HR, 1) * f
        wts = [f / tot for f in fac]
        for r in range(HR):
            acc = jnp.zeros((HL, D), F32)
            for s in range(NG):
                acc = acc + orecv[s, half, r] * wts[s][:, r:r + 1]
            q3[half * HR + r] = acc
        flatten(half)

    def flatten(half):
        at = slice(half * HR, half * HR + HR)
        for hh in range(HL):
            o2[at, hh * D:(hh + 1) * D] = q3[at, hh, :].astype(BF16)

    def d2d(k, g, half):
        at = pl.ds(half * HR, HR)
        return remote(p0.at[g, at], rb1.at[k, g, at], a_send.at[0], a_recv.at[k % 2, g, half], sib)

    def ycp(k, g, half):
        at = pl.ds(half * HR, HR)
        return remote(s1.at[g, at], rb2.at[k, g, at], y_send.at[0], y_recv.at[k % 2, g, half], ypeer)

    def back(k, g, half):
        at = pl.ds(half * HR, HR)
        return remote(t1.at[g, at], rb3.at[k, g, at], b_send.at[0], b_recv.at[k % 2, g, half], sib)

    def add_core(k, g, half):
        at = slice(half * HR, half * HR + HR)
        d2d(k, g, half).wait_recv()
        s1[g, at] = m0[g, at] + rb1[k, g, at]
        ycp(k, g, half).start()

    def add_chip(k, g, half):
        at = slice(half * HR, half * HR + HR)
        ycp(k, g, half).wait_recv()
        t1[g, at] = s1[g, at] + rb2[k, g, at]
        back(k, g, half).start()

    def settle(k, half, scale_col):
        at = slice(half * HR, half * HR + HR)

        def upd(src, c0):
            to = pl.ds(c0, HC)
            v = src if scale_col is None else scale_col[at] * src
            h[at, to] = (h[at, to] + v).astype(BF16).astype(F32)
        for g in range(NG):
            upd(t1[g, at], half_col(g, core))
        for g in range(NG):
            back(k, g, half).wait_recv()
            upd(rb3[k, g, at], half_col(g, other))

    def sent(ref, sem):
        pltpu.make_async_copy(ref, ref, sem.at[0]).wait()

    def drain(k):
        for ref, sem in ((p0, a_send), (s1, y_send), (t1, b_send)):
            sent(ref, sem)

    def o_products(k, seg, half, last):
        at = slice(half * HR, half * HR + HR)
        for g in range(NG):
            slot = slot_of(seg, g // 2)
            if half == 0 and g % 2 == 0:
                wait_pair(seg, g // 2)
            r = [jnp.dot(o2[at, :], slots[slot, g % 2, n * QW:(n + 1) * QW, :], **WIN) for n in range(4)]
            p0[g, at] = jnp.concatenate(r[:2], axis=1)
            d2d(k, g, half).start()
            m0[g, at] = jnp.concatenate(r[2:], axis=1)
            if last and g % 2:
                refill(seg, g // 2, g // 2)

    def down_product(seg):
        def f(g, part):
            j = 2 * g + part
            slot = wait_pair(seg, j, FF)
            r = [big_dot(act, lambda k, w: slots[slot, n, pl.ds(k, w), :], FF) for n in range(2)]
            refill(seg, j, 0)
            return jnp.concatenate(r, axis=1)
        return f

    def reduce_down(k, seg):
        product = down_product(seg)

        def both(g):
            for half in range(2):
                add_core(k, g, half)

        def body(g, _):
            p0[g] = product(g, 0)
            for half in range(2):
                d2d(k, g, half).start()

            @pl.when(g > 0)
            def _():
                both(g - 1)
            m0[g] = product(g, 1)
            return 0
        lax.fori_loop(0, NG, body, 0)
        both(3)

    def gate_up(seg, gain):
        for half in range(2):
            norm_rows(h, gain, x, half * HR, HR)

        def body(j, first):
            slot = wait_pair(seg, j)
            gv, uv = [big_dot(x, lambda k, w: slots[slot, n, pl.ds(k, w), :], W).astype(BF16).astype(F32) for n in range(2)]
            refill(seg, j, first)
            act[:, pl.ds(pl.multiple_of(j * QC, QC), QC)] = (gv * (1.0 / (1.0 + jnp.exp(-gv))) * uv).astype(BF16)
        sub_loops(seg, body)

    rid = iota((R, D), 0)
    maskv = jnp.zeros((R, D), F32)
    for r in range(R):
        maskv = jnp.where(rid == r, mask_s[row0 + r].astype(F32), maskv)
    mask_col = maskv[:, 0:1]

    for n in range(2 * NG):
        attend_stage(n)
        if n < NG:
            go(kv_self(n + NG))
        else:
            go(kv_cross(n - NG))
    fin_wait([hcopy])
    for c in range(0, W, HC):
        h[:, c:c + HC] = x[:, c:c + HC].astype(F32)

    def groups(f, k, half):
        for g in range(NG):
            f(k, g, half)

    combine(0)
    o_products(0, 0, 0, False)
    groups(add_core, 0, 0)
    combine(1)
    o_products(0, 0, 1, True)
    groups(add_core, 0, 1)
    groups(add_chip, 0, 0)
    settle(0, 0, None)
    groups(add_chip, 0, 1)
    settle(0, 1, None)
    drain(0)
    gate_up(1, g2)

    reduce_down(1, 2)
    for g in range(NG):
        for half in range(2):
            add_chip(1, g, half)
    for half in range(2):
        settle(1, half, None)
    drain(1)

    for half in range(2):
        norm_rows(h, g3, x, half * HR, HR)
    for j in range(2):
        slot = wait_pair(3, j)
        ys = [big_dot(x, lambda k, w: slots[slot, n, pl.ds(k, w), :], W).astype(BF16).astype(F32) for n in range(2)]
        refill(3, j, j)
        for hh in range(4):
            t = ys[hh // 2][:, hh % 2 * D:(hh % 2 + 1) * D]
            inv = lax.rsqrt(jnp.mean(t * t, axis=-1, keepdims=True) + NORM_EPS)
            q3[:, NG * j + hh, :] = (t * inv * qn[...].astype(F32)).astype(BF16).astype(F32)
    fin_wait([xcopy])
    xlen = jnp.sum(jnp.where(xv[...] > 0, 1.0, 0.0), axis=-1, keepdims=True)
    xl[...] = jnp.broadcast_to(2.0 * xlen, (R, D))
    lane2 = iota((HL, 2 * D), 1)
    par2 = (lane2 % 2) == (iota((HL, 2 * D), 0) // 4)
    lanef = lane2.astype(F32)

    for half in range(2):
        fin_wait(kv_cross(2 * half) + kv_cross(2 * half + 1))

        def xbody(it, _):
            res = []
            for u in range(HL):
                v = it * HL + u
                b = half * HR + v
                s = jnp.concatenate([scores(q3[b], kb[2 * half + t, v]) for t in range(2)], axis=1)
                ok = par2 & (lanef < xl[pl.ds(b, 1), :][:, 0:1])
                s = jnp.where(ok, s, NEG_BIG)
                m = jnp.max(s, axis=-1, keepdims=True)
                p = jnp.where(ok, jnp.exp(s - m), 0.0)
                res.append((p, jnp.sum(p, axis=-1, keepdims=True)))
            for u in range(HL):
                v = it * HL + u
                p, l = res[u]
                o = sum(jnp.dot(p[:, t * D:(t + 1) * D].astype(BF16), vb[2 * half + t, v], **WIN) for t in range(2))
                q3[half * HR + v] = o / l
            return 0
        lax.fori_loop(0, HR // HL, xbody, 0)
        flatten(half)
        if half:
            groups(add_core, 2, 0)
        o_products(2, 4, half, half == 1)
    groups(add_core, 2, 1)

    ga = jnp.tanh(jnp.full((R, 1), gates[0], F32)) * mask_col
    gm2 = jnp.tanh(jnp.full((R, 1), gates[1], F32)) * mask_col
    groups(add_chip, 2, 0)
    settle(2, 0, ga)
    groups(add_chip, 2, 1)
    settle(2, 1, ga)
    drain(2)
    gate_up(5, g4)

    product = down_product(6)

    def quarter(y):
        return pl.ds(pl.multiple_of(y * QC, QC), QC)

    def last_d2d(g):
        return remote(p0.at[g], rb1.at[3, g], a_send.at[0], a_recv.at[1, g, 0], sib)

    def qcp(g):
        return remote(s1.at[g, :, quarter(1 - ypos)], rbq.at[g], y_send.at[0], y_recv.at[1, g, 0], ypeer)

    def zcp(g, d):
        piece = fin.at[g, core, ypos, sp]
        return remote(piece, piece, z_send.at[0], z_recv.at[g, d], {'sp': (sp + d) % NG})

    def fcp(g, d):
        z = (sp + NG - d) % NG
        piece = fin.at[g, core, ypos, z]
        return remote(piece, piece, f_send.at[0], f_recv.at[g, d], ypeer)

    def ecp(g):
        piece = fin.at[g, core]
        return remote(piece, piece, e_send.at[0], e_recv.at[g], sib)

    def stage_q(g):
        qcp(g).wait_recv()
        c0 = pl.multiple_of(half_col(g, core) + ypos * QC, QC)
        t = s1[g, :, quarter(ypos)] + rbq[g]
        fin[g, core, ypos, sp] = (h[:, pl.ds(c0, QC)] + gm2 * t).astype(BF16).astype(F32)
        for d in NEAR:
            zcp(g, d).start()
        fcp(g, 0).start()

    def stage_f(g):
        for d in NEAR:
            zcp(g, d).wait_recv()
            fcp(g, d).start()

    def emit(g, half):
        for yy in range(2):
            c = pl.multiple_of(half_col(g, half) + yy * QC, QC)
            for zz in range(NG):
                ov[zz * R:(zz + 1) * R, pl.ds(c, QC)] = fin[g, half, yy, zz].astype(BF16)

    def out_copy(g, n):
        at = pl.ds(half_col(g, (core, other)[n]), HC)
        return pltpu.make_async_copy(ov.at[:, at], out.at[:, at], v_sem.at[0])

    def stage_e(g):
        for d in (0,) + NEAR:
            fcp(g, d).wait_recv()
        ecp(g).start()
        emit(g, core)
        out_copy(g, 0).start()

    def stage_c(g):
        last_d2d(g).wait_recv()
        s1[g] = m0[g] + rb1[3, g]
        qcp(g).start()

    def body(g, _):
        p0[g] = product(g, 0)
        last_d2d(g).start()

        @pl.when(g > 0)
        def _():
            stage_c(g - 1)
        m0[g] = product(g, 1)

        @pl.when(g > 1)
        def _():
            stage_q(g - 2)
        return 0
    lax.fori_loop(0, NG, body, 0)
    stage_c(3)
    stage_q(2)
    stage_q(3)
    stage_f(0)
    stage_f(1)
    stage_e(0)
    stage_f(2)
    stage_e(1)
    stage_f(3)
    stage_e(2)
    stage_e(3)

    for g in range(NG):
        ecp(g).wait_recv()
        emit(g, other)
        out_copy(g, 1).start()
    pltpu.make_async_copy(ov, out, v_sem.at[0]).wait()
    sent(ob.at[1:NG], sp_send)
    sent(p0, a_send)
    sent(s1.at[:, :, 0:QC], y_send)
    sent(fin.at[0:3, 0, 0], z_send)
    sent(fin.at[:, 0, 0], f_send)
    sent(fin.at[:, 0], e_send)


def solution(mesh):
    cache_spec = P('dp', 'sp', 'tp', None)
    cross_spec = P('dp', None, 'tp', None)
    row_spec = P('dp', None)
    vec_spec = P('dp')
    full_spec = P(None)
    col_spec = P(None, 'tp')
    split_rows = P('tp', None)
    in_specs = (row_spec, vec_spec, cache_spec, cache_spec, cross_spec, cross_spec, row_spec, vec_spec,
                full_spec, col_spec, col_spec, col_spec, split_rows, full_spec, col_spec, col_spec, split_rows,
                full_spec, col_spec, full_spec, split_rows, full_spec, full_spec, col_spec, col_spec, split_rows)
    out_specs = (row_spec, cache_spec, cache_spec)
    vm = pl.BlockSpec(memory_space=VMEM)
    sm = pl.BlockSpec(memory_space=SMEM)
    an = pl.BlockSpec(memory_space=ANY)
    dma = pltpu.SemaphoreType.DMA

    def local_step(hidden, new_pos, k_self, v_self, k_cross, v_cross, xvalid, rowmask,
                   self_attn_norm, self_wq, self_wk, self_wv, self_wo, self_mlp_norm,
                   self_wgate, self_wup, self_wdown, cross_attn_norm, cross_wq, cross_qnorm,
                   cross_wo, cross_gates, cross_mlp_norm, cross_wgate, cross_wup, cross_wdown):
        kc = k_self.reshape(B, D, D)
        vc = v_self.reshape(B, D, D)
        cache = jax.ShapeDtypeStruct((B, D, D), BF16)
        kout, vout, q = pl.pallas_call(
            self_kernel,
            name='self_part',
            out_shape=(cache, cache, jax.ShapeDtypeStruct((B, HL, D), F32)),
            in_specs=[sm, vm] + [an] * 7,
            out_specs=(an, an, an),
            scratch_shapes=[VMEM((B, W), BF16), VMEM((B, W), BF16), VMEM((6, W, QC), BF16),
                            VMEM((B, D, D), BF16), VMEM((B, D, D), BF16),
                            VMEM((B, HL, D), F32), VMEM((2, B, D), F32), VMEM((2, B, D), F32),
                            VMEM((B, D), F32), VMEM((B, D), F32), VMEM((1, D), I32),
                            dma((6,)), dma((8,)), dma((8,)), dma((3,))],
            compiler_params=pltpu.CompilerParams(vmem_limit_bytes=MAXV),
        )(new_pos, self_attn_norm.reshape(R, D), new_pos[None, :], hidden, self_wq, self_wk, self_wv, kc, vc)

        part = VMEM((NG, R, HC), F32)
        parts3 = VMEM((3, NG, R, HC), F32)
        h4 = pl.pallas_call(
            rest_kernel,
            name='rest_part',
            out_shape=jax.ShapeDtypeStruct((B, W), BF16),
            in_specs=[sm, sm, sm, vm, vm, vm, vm] + [an] * 16,
            out_specs=an,
            scratch_shapes=[
                VMEM((NP, 2, W, QC), BF16), VMEM((B, HL, D), F32), VMEM((NG, 2, HR + 1, HL, D), F32),
                VMEM((NG, 2, HR + 1, HL, D), F32),
                VMEM((R, W), F32), VMEM((R, W), BF16), VMEM((R, FF), BF16), VMEM((R, QW), BF16),
                VMEM((R, HL, D), F32), VMEM((NG, HR, D, D), BF16), VMEM((NG, HR, D, D), BF16),
                VMEM((R, D), I32), VMEM((R, D), F32),
                part, part, part, part,
                VMEM((4, NG, R, HC), F32), parts3, parts3,
                VMEM((NG, R, QC), F32), VMEM((NG, 2, 2, NG, R, QC), F32), VMEM((B, W), BF16), dma((1,)), dma((2 * NG,)),
                dma((NP,)), dma((3,)), dma((2, NG)), dma((1,)), dma((2, NG)),
                dma((1,)), dma((2, NG, 2)), dma((1,)), dma((2, NG, 2)), dma((1,)), dma((2, NG, 2)),
                dma((1,)), dma((NG, NG)), dma((1,)), dma((NG, NG)), dma((1,)), dma((NG,))],
            compiler_params=pltpu.CompilerParams(collective_id=0, has_side_effects=True,
                                                 vmem_limit_bytes=MAXV),
        )(new_pos, rowmask, cross_gates, self_mlp_norm.reshape(R, D), cross_attn_norm.reshape(R, D),
          cross_mlp_norm.reshape(R, D), cross_qnorm[None, :], q, kout, vout, hidden, xvalid,
          k_cross.reshape(B, 2, D, D), v_cross.reshape(B, 2, D, D),
          self_wo, self_wgate, self_wup, self_wdown, cross_wq, cross_wo, cross_wgate, cross_wup, cross_wdown)
        return h4, kout.reshape(k_self.shape), vout.reshape(v_self.shape)

    return jax.shard_map(local_step, mesh=mesh, in_specs=in_specs, out_specs=out_specs, check_vma=False)
```
